32 devices in a mesh: row: 4 (over y, x), col: 8 (over z, core).
Axes of the slice: x: 2, y: 2, z: 4, core: 2. Of those that a mesh axis runs over, the one named last changes fastest.
Arguments:
- view_one: bfloat16 [2048, 8192], P('row', 'col'), may hold values from -6 to 6
- view_two: bfloat16 [2048, 8192], P('row', 'col'), may hold values from -6 to 6
- pair_weights: bfloat16 [8192, 8192], P('row', 'col'), may hold values from 0.25 to 2.5
Outputs:
- first_grad: bfloat16 [2048, 8192], P('row', 'col')
- second_grad: bfloat16 [2048, 8192], P('row', 'col')
The draws below stay inside these ranges and needn't reach their ends.
All inputs are finite; a program needn't handle non-finite values.
Results may differ from the reference program's by a relative error of at most 0.004.
Values may be sent and summed in bfloat16 or wider, within the bound.
A program may use at most 128 MiB of HBM per device.

```python
import math
import jax
import jax.numpy as jnp

D = 8192
BATCH = 2048


def block_levels(own_key, shape, shards, least, high):
    factor_of, own = 1.0, jax.random.fold_in(own_key, 6)
    for position, shards_of in shards:
        heights = jnp.exp(jax.random.uniform(jax.random.fold_in(own, position), (shards_of,), jnp.float32, least / len(shards), high / len(shards)))
        factor_of = factor_of * jnp.repeat(heights, shape[position] // shards_of).reshape([-1 if axis == position else 1 for axis in range(len(shape))])
    return factor_of


def centred(key, shape, scale, bound, cuts=(), held_as=jnp.bfloat16):
    drawn = scale * jax.random.normal(key, shape, jnp.float32)
    if cuts:
        drawn = drawn * block_levels(key, shape, cuts, -0.22, 0.18)
    return jnp.clip(drawn, -bound, bound).astype(held_as)


def setup_inputs(seed: int = 0) -> dict:
    seeds = jax.random.split(jax.random.key(seed), 4)
    return {
        "view_one": centred(seeds[0], (BATCH, D), 1.0, 6.0, ((0, 4), (1, 8))),
        "view_two": centred(seeds[1], (BATCH, D), 1.0, 6.0, ((0, 4), (1, 8))),
        "pair_weights": jnp.clip(jnp.exp(math.log(2.5) - 2.3025851 * jax.random.uniform(seeds[2], (D, D), jnp.float32) ** block_levels(seeds[2], (D, D), ((0, 4), (1, 8)), -0.2, 0.2)), 0.25, 2.5).astype(jnp.bfloat16),
    }


def reference(view_one, view_two, pair_weights):
    samples = view_one.shape[0]
    correlation = jnp.dot(view_two.T, view_one, preferred_element_type=jnp.float32) / samples
    identity = jnp.eye(D, dtype=jnp.float32)
    weighted = (pair_weights.astype(jnp.float32) * (correlation - identity)).astype(jnp.bfloat16)
    first_grad = jnp.dot(view_two, weighted, preferred_element_type=jnp.float32).astype(jnp.bfloat16)
    second_grad = jnp.dot(view_one, weighted.T, preferred_element_type=jnp.float32).astype(jnp.bfloat16)
    return first_grad, second_grad
```

```python
import jax
import jax.numpy as jnp
from jax import lax
from jax.experimental import pallas as pl
from jax.experimental.pallas import tpu as pltpu
from jax.sharding import PartitionSpec as P

MESH = pl.DeviceIdType.MESH
CORES = 2
HALVES = 2
PAIR = 2


def arrived(ref, sem):
    pltpu.make_async_copy(ref, ref, sem).wait()


def remote(src, dst, send, recv, device):
    return pltpu.make_async_remote_copy(
        src_ref=src, dst_ref=dst, send_sem=send, recv_sem=recv, device_id=device, device_id_type=MESH
    )


def at(start, size):
    return pl.ds(pl.multiple_of(start, size), size)


def pick(index, values):
    chosen = jnp.int32(values[0])
    for i, value in enumerate(values[1:], 1):
        chosen = jnp.where(index == i, value, chosen)
    return chosen


def step_kernel(rows, strip, one_ref, two_ref, pair_ref, first_out, second_out, two_held, two_own, two_twin, turned, one,
                pair, weighted, theirs, below, above, second_sent, second_sum, first_sent, first_wide, first_deep,
                wide_sum, deep_sum, load_sem, two_recv, feed_send, up_send, down_send, two_pair, one_send, one_recv,
                one_pair, weight_sem, theirs_sem, chain_send, below_recv, above_recv, spread_send, spread_recv,
                first_send, wide_recv, deep_recv, wide_last, deep_last):
    samples, width = two_ref.shape
    wide = PAIR
    deep = rows // wide
    strips = width // strip
    part = samples // HALVES
    chunk = rows * HALVES
    pieces = strips * chunk
    tile = min(width, 512)
    tiles = width // tile
    parts = CORES * tiles
    row, col = lax.axis_index("row"), lax.axis_index("col")
    z, core = lax.div(col, CORES), lax.rem(col, CORES)
    other = 1 - core
    a, b = lax.rem(row, wide), lax.div(row, wide)
    home = z == row
    reach = jnp.where(z > row, rows - 1 - row, jnp.where(z < row, row, jnp.maximum(row, rows - 1 - row)))
    back = reach - jnp.abs(z - row)
    last = back == 0
    twin = (row, col + 1 - 2 * core)

    def device(target, level):
        return (target, level * CORES + core)

    def half(h):
        return at(h * part, part)

    def cols(q):
        return at(q * strip, strip)

    def split(t):
        return lax.div(t, chunk), lax.rem(lax.div(t, HALVES), rows), lax.rem(t, HALVES)

    def two_piece(t):
        q, i, h = split(t)
        return two_own.at[lax.rem(row + i, rows), half(h), cols(q)]

    def two_up(t):
        return remote(two_piece(t), two_piece(t), up_send.at[t], two_recv.at[t], device(row, z + 1))

    def two_down(t):
        return remote(two_piece(t), two_piece(t), down_send.at[t], two_recv.at[t], device(row, z - 1))

    def feed(q, h):
        t = q * chunk + lax.rem(row - z + rows, rows) * HALVES + h
        return remote(two_held.at[half(h), cols(q)], two_own.at[row, half(h), cols(q)], feed_send.at[q, h],
                      two_recv.at[t], device(z, z))

    def own_two(q, h):
        return pltpu.make_async_copy(two_ref.at[half(h), cols(q)], two_own.at[row, half(h), cols(q)],
                                     two_recv.at[q * chunk + h])

    def feeds(q):
        @pl.when(z != row)
        def _():
            for h in range(HALVES):
                feed(q, h).start()

    def two_swap(q):
        return remote(two_own.at[:, :, cols(q)], two_twin.at[:, :, cols(q)], two_pair.at[0, q], two_pair.at[1, q], twin)

    def one_block(block, h):
        return one.at[core, block, half(h)]

    def one_copy(block, h, target):
        return remote(one_block(block, h), one_block(block, h), one_send.at[block, h, target], one_recv.at[block, h],
                      (target, col))

    def one_swap(block, h):
        return remote(one_block(block, h), one_block(block, h), one_pair.at[0, block, h], one_pair.at[1, block, h],
                      twin)

    def block_of(over, down):
        return lax.rem(b + down, deep) * wide + lax.rem(a + over, wide)

    across = [(over, 0) for over in range(1, wide)]
    along = [(0, down) for down in range(1, deep)]
    far = [(over, down) for over in range(1, wide) for down in range(1, deep)]

    def take_one(block, h):
        arrived(one_block(block, h), one_recv.at[block, h])
        one_swap(block, h).start()

    def weights_swap():
        return remote(pair_ref.at[at(other * width, width)], pair.at[core], weight_sem.at[0], weight_sem.at[1], twin)

    def theirs_swap(q):
        return remote(weighted.at[other, cols(q)], theirs.at[cols(q)], theirs_sem.at[0, q], theirs_sem.at[1, q], twin)

    load_two = pltpu.make_async_copy(two_ref, two_held, load_sem.at[0])
    load_one = pltpu.make_async_copy(one_ref, one.at[core, row], load_sem.at[1])
    load_pair = pltpu.make_async_copy(pair_ref.at[at(core * width, width)], pair.at[core], load_sem.at[2])

    load_two.start()

    @pl.when(home)
    def _():
        for q in range(strips):
            for h in range(HALVES):
                own_two(q, h).start()

    load_one.start()
    load_pair.start()
    load_two.wait()
    feeds(0)
    load_one.wait()
    for h in range(HALVES):
        for over, down in across:
            one_copy(row, h, block_of(over, down)).start()
        for over, down in along:
            one_copy(row, HALVES - 1 - h, block_of(over, down)).start()
    for h in range(HALVES):
        one_swap(row, h).start()
    weights_swap().start()
    if strips > 1:
        feeds(1)

    def relay_one():
        for over, down in across:
            block = block_of(over, down)
            take_one(block, 0)
            for _, other_down in along:
                one_copy(block, 0, block_of(0, other_down)).start()
        for over, down in along:
            block = block_of(over, down)
            take_one(block, 1)
            for other_over, _ in across:
                one_copy(block, 1, block_of(other_over, 0)).start()
        for q in range(2, strips):
            feeds(q)

    def finish_one():
        for over, down in across:
            take_one(block_of(over, down), 1)
        for over, down in along:
            take_one(block_of(over, down), 0)
        for over, down in far:
            take_one(block_of(over, down), 0)
            take_one(block_of(over, down), 1)
        for block in range(rows):
            for h in range(HALVES):
                arrived(one.at[other, block, half(h)], one_pair.at[1, block, h])
        load_pair.wait()
        arrived(pair.at[other], weight_sem.at[1])

    def correlate(q, p):
        side, i = lax.div(p, tiles), lax.rem(p, tiles)

        @pl.when(p == 0)
        def _():
            turned[...] = two_own[:, :, cols(q)].reshape(rows * samples, strip).T

        columns = at(i * tile, tile)
        total = jnp.dot(turned[...], one[side, :, :, columns].reshape(rows * samples, tile),
                        preferred_element_type=jnp.float32)
        row_ids = (row * CORES + core) * width + q * strip + lax.broadcasted_iota(jnp.int32, total.shape, 0)
        col_ids = (z * CORES + side) * width + i * tile + lax.broadcasted_iota(jnp.int32, total.shape, 1)
        identity = jnp.where(row_ids == col_ids, 1.0, 0.0).astype(jnp.float32)
        scale = pair[side, cols(q), columns].astype(jnp.float32)
        weighted[side, cols(q), columns] = (scale * (total / (rows * samples) - identity)).astype(jnp.bfloat16)

        @pl.when(p == parts - 1)
        def _():
            theirs_swap(q).start()

    def chain_up(g):
        return remote(second_sent.at[g], below.at[g], chain_send.at[g], below_recv.at[g], device(row, z + 1))

    def chain_down(g):
        return remote(second_sent.at[g], above.at[g], chain_send.at[g], above_recv.at[g], device(row, z - 1))

    def spread(g):
        q, i, h = split(g)
        return remote(second_sent.at[g], second_out.at[half(h), cols(q)], spread_send.at[g], spread_recv.at[q, h],
                      device(lax.rem(row + 1 + i, rows), z))

    from_below = jnp.logical_and(z > 0, z <= row)
    from_above = jnp.logical_and(z < rows - 1, z >= row)

    def second_piece(g):
        q, i, h = split(g)
        target = lax.rem(row + 1 + i, rows)
        contract = (((1,), (1,)), ((), ()))
        second_sum[...] = (
            lax.dot_general(one[0, target, half(h)], weighted[0, cols(q)], contract, preferred_element_type=jnp.float32)
            + lax.dot_general(one[1, target, half(h)], weighted[1, cols(q)], contract,
                              preferred_element_type=jnp.float32))

        @pl.when(from_below)
        def _():
            arrived(below.at[g], below_recv.at[g])
            second_sum[...] += below[g].astype(jnp.float32)

        @pl.when(from_above)
        def _():
            arrived(above.at[g], above_recv.at[g])
            second_sum[...] += above[g].astype(jnp.float32)

        keep = jnp.logical_and(home, i == rows - 1)

        @pl.when(keep)
        def _():
            second_out[half(h), cols(q)] = second_sum[...].astype(jnp.bfloat16)

        @pl.when(jnp.logical_not(keep))
        def _():
            second_sent[g] = second_sum[...].astype(jnp.bfloat16)

        @pl.when(z < row)
        def _():
            chain_up(g).start()

        @pl.when(z > row)
        def _():
            chain_down(g).start()

        @pl.when(jnp.logical_and(home, i != rows - 1))
        def _():
            spread(g).start()

    lead = [(0, over, down) for over, _ in across for down in range(deep)]
    lead_deep = [(1, over, down) for _, down in along for over in range(wide)]
    order = []
    for i in range(max(len(lead), len(lead_deep))):
        order += lead[::-1][i:i + 1] + lead_deep[::-1][i:i + 1]
    opening = len(order)
    order += [(0, 0, down) for _, down in along] + [(1, over, 0) for over, _ in across] + [(0, 0, 0), (1, 0, 0)]

    def unit(u):
        h = pick(u, [entry[0] for entry in order])
        over = pick(u, [entry[1] for entry in order])
        down = pick(u, [entry[2] for entry in order])
        return h, over, down, block_of(over, down)

    def first_hop(u):
        h, over, down, target = unit(u)
        flat = jnp.where(h == 0, (over - 1) * deep + lax.div(target, wide), (down - 1) * wide + lax.rem(target, wide))
        return h, over, down, target, flat

    def wide_open(u):
        h, over, down, target, flat = first_hop(u)
        return remote(first_sent.at[target, half(h)], first_wide.at[flat], first_send.at[u], wide_recv.at[flat],
                      (b * wide + lax.rem(a + over, wide), col))

    def deep_open(u):
        h, over, down, target, flat = first_hop(u)
        return remote(first_sent.at[target, half(h)], first_deep.at[flat], first_send.at[u], deep_recv.at[flat],
                      (lax.rem(b + down, deep) * wide + a, col))

    def deep_close(u):
        h, over, down, target = unit(u)
        return remote(first_sent.at[target, half(h)], deep_sum.at[down - 1], first_send.at[u], deep_last.at[down - 1],
                      (target, col))

    def wide_close(u):
        h, over, down, target = unit(u)
        return remote(first_sent.at[target, half(h)], wide_sum.at[over - 1], first_send.at[u], wide_last.at[over - 1],
                      (target, col))

    def first_tile(target, h, columns):
        return (jnp.dot(two_own[target, half(h)], weighted[core, :, columns], preferred_element_type=jnp.float32)
                + jnp.dot(two_twin[target, half(h)], theirs[:, columns], preferred_element_type=jnp.float32))

    def first_opening(u):
        h, over, down, target = unit(u)

        def body(i, _):
            columns = at(i * tile, tile)
            first_sent[target, half(h), columns] = first_tile(target, h, columns).astype(jnp.bfloat16)
            return 0

        lax.fori_loop(0, tiles, body, 0)

        @pl.when(h == 0)
        def _():
            wide_open(u).start()

        @pl.when(h == 1)
        def _():
            deep_open(u).start()

    def first_closing(u):
        h, over, down, target = unit(u)

        @pl.when(h == 0)
        def _():
            for over_ in range(1, wide):
                flat = (over_ - 1) * deep + lax.div(target, wide)
                arrived(first_wide.at[flat], wide_recv.at[flat])

        @pl.when(h == 1)
        def _():
            for down_ in range(1, deep):
                flat = (down_ - 1) * wide + lax.rem(target, wide)
                arrived(first_deep.at[flat], deep_recv.at[flat])

        def body(i, _):
            columns = at(i * tile, tile)
            total = first_tile(target, h, columns)

            @pl.when(h == 0)
            def _():
                acc = total
                for over_ in range(1, wide):
                    acc += first_wide[(over_ - 1) * deep + lax.div(target, wide), :, columns].astype(jnp.float32)
                first_sent[target, half(h), columns] = acc.astype(jnp.bfloat16)

            @pl.when(h == 1)
            def _():
                acc = total
                for down_ in range(1, deep):
                    acc += first_deep[(down_ - 1) * wide + lax.rem(target, wide), :, columns].astype(jnp.float32)
                first_sent[target, half(h), columns] = acc.astype(jnp.bfloat16)

            return 0

        lax.fori_loop(0, tiles, body, 0)

        @pl.when(h == 0)
        def _():
            deep_close(u).start()

        @pl.when(h == 1)
        def _():
            wide_close(u).start()

    closing = len(order) - 2 - opening
    lag = jnp.where(last, 0, jnp.minimum(6, 4 * back - 2))
    second_lag = chunk - 1 + jnp.where(last, 0, 2 + 4 * back)
    done = jnp.where(last, pieces, pieces - 1 + lag + parts)
    open_slot = done + 1
    close_slot = jnp.maximum(open_slot + 2, pieces + 8 + 2 * back)
    relay_slot = jnp.maximum(0, 4 - 2 * jnp.abs(z - row))
    slots = pieces + chunk + 2 + 4 * rows
    each = (opening + 1) // 2

    def slot(t, _):
        @pl.when(t == relay_slot)
        def _():
            relay_one()

        @pl.when(t < pieces)
        def _():
            arrived(two_piece(t), two_recv.at[t])

            @pl.when(jnp.logical_and(z >= row, z < rows - 1))
            def _():
                two_up(t).start()

            @pl.when(jnp.logical_and(z <= row, z > 0))
            def _():
                two_down(t).start()

            @pl.when(lax.rem(t, chunk) == chunk - 1)
            def _():
                two_swap(lax.div(t, chunk)).start()

        since = t - (chunk - 1) - lag

        @pl.when(since == 0)
        def _():
            finish_one()

        q, p = lax.div(since, chunk), lax.rem(since, chunk)
        live = jnp.logical_and(since >= 0, q < strips)
        low = jnp.where(jnp.logical_or(last, jnp.logical_not(live)), 0, p)
        high = jnp.where(last, jnp.where(p == 0, parts, 0), jnp.where(p < parts, p + 1, 0))
        high = jnp.where(live, high, 0)

        def piece(i, _):
            correlate(q, i)
            return 0

        lax.fori_loop(low, high, piece, 0)

        @pl.when(t == open_slot)
        def _():
            for q_ in range(strips):
                arrived(two_twin.at[:, :, cols(q_)], two_pair.at[1, q_])
                arrived(theirs.at[cols(q_)], theirs_sem.at[1, q_])

        g = t - second_lag

        @pl.when(jnp.logical_and(g >= 0, g < pieces))
        def _():
            second_piece(g)

        first = jnp.where(t == open_slot, 0, jnp.where(t == open_slot + 1, each, opening))
        final = jnp.where(t == open_slot, each, opening)

        def opener(u, _):
            first_opening(u)
            return 0

        lax.fori_loop(first, final, opener, 0)

        def closer(u, _):
            first_closing(u)
            return 0

        lax.fori_loop(opening, jnp.where(t == close_slot, opening + closing, opening), closer, 0)
        return 0

    lax.fori_loop(0, slots, slot, 0)

    for _, down in along:
        arrived(deep_sum.at[down - 1], deep_last.at[down - 1])
    for over, _ in across:
        arrived(wide_sum.at[over - 1], wide_last.at[over - 1])
        for d in range(deep):
            @pl.when(d == b)
            def _(over=over, d=d):
                flat = (over - 1) * deep + d
                arrived(first_wide.at[flat], wide_recv.at[flat])
    for _, down in along:
        for o in range(wide):
            @pl.when(o == a)
            def _(down=down, o=o):
                flat = (down - 1) * wide + o
                arrived(first_deep.at[flat], deep_recv.at[flat])

    def finish_first(i, _):
        columns = at(i * tile, tile)
        top = first_tile(row, 0, columns)
        for over, _ in across:
            top += first_wide[(over - 1) * deep + b, :, columns].astype(jnp.float32)
        for _, down in along:
            top += deep_sum[down - 1, :, columns].astype(jnp.float32)
        first_out[half(0), columns] = top.astype(jnp.bfloat16)
        low = first_tile(row, 1, columns)
        for _, down in along:
            low += first_deep[(down - 1) * wide + a, :, columns].astype(jnp.float32)
        for over, _ in across:
            low += wide_sum[over - 1, :, columns].astype(jnp.float32)
        first_out[half(1), columns] = low.astype(jnp.bfloat16)
        return 0

    lax.fori_loop(0, tiles, finish_first, 0)

    @pl.when(z != row)
    def _():
        for q in range(strips):
            for h in range(HALVES):
                arrived(second_out.at[half(h), cols(q)], spread_recv.at[q, h])
                feed(q, h).wait_send()

    def settle(t, _):
        q, i, h = split(t)

        @pl.when(jnp.logical_and(z >= row, z < rows - 1))
        def _():
            two_up(t).wait_send()

        @pl.when(jnp.logical_and(z <= row, z > 0))
        def _():
            two_down(t).wait_send()

        @pl.when(z < row)
        def _():
            chain_up(t).wait_send()

        @pl.when(z > row)
        def _():
            chain_down(t).wait_send()

        @pl.when(jnp.logical_and(home, i != rows - 1))
        def _():
            spread(t).wait_send()

        return 0

    lax.fori_loop(0, pieces, settle, 0)
    for q in range(strips):
        two_swap(q).wait_send()
        theirs_swap(q).wait_send()
    weights_swap().wait_send()
    for h in range(HALVES):
        for over, down in across + along:
            one_copy(row, h, block_of(over, down)).wait_send()
        for block in range(rows):
            one_swap(block, h).wait_send()
    for over, down in across:
        for _, other_down in along:
            one_copy(block_of(over, down), 0, block_of(0, other_down)).wait_send()
    for over, down in along:
        for other_over, _ in across:
            one_copy(block_of(over, down), 1, block_of(other_over, 0)).wait_send()

    def settle_first(u, _):
        h, over, down, target = unit(u)
        arrived(first_sent.at[target, half(h)], first_send.at[u])
        return 0

    lax.fori_loop(0, opening + closing, settle_first, 0)


def per_device(view_one, view_two, pair_weights):
    rows = lax.axis_size("row")
    samples, width = view_one.shape
    strip = min(width, 256)
    strips = width // strip
    wide, deep = PAIR, rows // PAIR
    part = samples // HALVES
    pieces = strips * rows * HALVES
    units = 2 * rows
    own = jax.ShapeDtypeStruct((samples, width), jnp.bfloat16)
    any_space = pl.BlockSpec(memory_space=pl.ANY)
    vmem = pl.BlockSpec(memory_space=pltpu.VMEM)
    dma = pltpu.SemaphoreType.DMA

    def held(*shape):
        return pltpu.VMEM(shape, jnp.bfloat16)

    crossing = (wide - 1) * deep
    descent = (deep - 1) * wide
    return pl.pallas_call(
        lambda *refs: step_kernel(rows, strip, *refs),
        out_shape=(own, own),
        in_specs=[any_space] * 3,
        out_specs=(vmem, vmem),
        scratch_shapes=[
            held(samples, width),
            held(rows, samples, width),
            held(rows, samples, width),
            held(strip, rows * samples),
            held(CORES, rows, samples, width),
            held(CORES, width, width),
            held(CORES, width, width),
            held(width, width),
            held(pieces, part, strip),
            held(pieces, part, strip),
            held(pieces, part, strip),
            pltpu.VMEM((part, strip), jnp.float32),
            held(rows, samples, width),
            held(crossing, part, width),
            held(descent, part, width),
            held(wide - 1, part, width),
            held(deep - 1, part, width),
            dma((3,)),
            dma((pieces,)),
            dma((strips, HALVES)),
            dma((pieces,)),
            dma((pieces,)),
            dma((2, strips)),
            dma((rows, HALVES, rows)),
            dma((rows, HALVES)),
            dma((2, rows, HALVES)),
            dma((2,)),
            dma((2, strips)),
            dma((pieces,)),
            dma((pieces,)),
            dma((pieces,)),
            dma((pieces,)),
            dma((strips, HALVES)),
            dma((units,)),
            dma((crossing,)),
            dma((descent,)),
            dma((wide - 1,)),
            dma((deep - 1,)),
        ],
        compiler_params=pltpu.CompilerParams(has_side_effects=True, vmem_limit_bytes=62 * 2**20),
        name="twins_step",
    )(view_one, view_two, pair_weights)


def solution(mesh):
    placed = (P("row", "col"), P("row", "col"), P("row", "col"))
    return jax.shard_map(
        per_device,
        mesh=mesh,
        in_specs=placed,
        out_specs=(P("row", "col"), P("row", "col")),
        check_vma=False,
    )
```

```python
import jax
import jax.numpy as jnp
from jax import lax
from jax.experimental import pallas as pl
from jax.experimental.pallas import tpu as pltpu
from jax.sharding import PartitionSpec as P

MESH = pl.DeviceIdType.MESH
CORES = 2
HALVES = 2
PAIR = 2


def arrived(ref, sem):
    pltpu.make_async_copy(ref, ref, sem).wait()


def remote(src, dst, send, recv, device):
    return pltpu.make_async_remote_copy(
        src_ref=src, dst_ref=dst, send_sem=send, recv_sem=recv, device_id=device, device_id_type=MESH
    )


def at(start, size):
    return pl.ds(pl.multiple_of(start, size), size)


def pick(index, values):
    chosen = jnp.int32(values[0])
    for i, value in enumerate(values[1:], 1):
        chosen = jnp.where(index == i, value, chosen)
    return chosen


def step_kernel(rows, strip, one_ref, two_ref, pair_ref, first_out, second_out, two_held, two_own, two_twin, turned, one,
                pair, weighted, theirs, below, above, second_sent, second_sum, first_sent, first_wide, first_deep,
                wide_sum, deep_sum, load_sem, two_recv, feed_send, up_send, down_send, two_pair, one_send, one_recv,
                one_pair, weight_sem, theirs_sem, chain_send, below_recv, above_recv, spread_send, spread_recv,
                first_send, wide_recv, deep_recv, wide_last, deep_last):
    samples, width = two_ref.shape
    wide = PAIR
    deep = rows // wide
    strips = width // strip
    part = samples // HALVES
    chunk = rows * HALVES
    pieces = strips * chunk
    tile = min(width, 512)
    tiles = width // tile
    parts = CORES * tiles
    row, col = lax.axis_index("row"), lax.axis_index("col")
    z, core = lax.div(col, CORES), lax.rem(col, CORES)
    other = 1 - core
    a, b = lax.rem(row, wide), lax.div(row, wide)
    home = z == row
    reach = jnp.where(z > row, rows - 1 - row, jnp.where(z < row, row, jnp.maximum(row, rows - 1 - row)))
    back = reach - jnp.abs(z - row)
    last = back == 0
    back = jnp.where(home, rows, back)
    twin = (row, col + 1 - 2 * core)

    def device(target, level):
        return (target, level * CORES + core)

    def half(h):
        return at(h * part, part)

    def cols(q):
        return at(q * strip, strip)

    def split(t):
        return lax.div(t, chunk), lax.rem(lax.div(t, HALVES), rows), lax.rem(t, HALVES)

    def two_piece(t):
        q, i, h = split(t)
        return two_own.at[lax.rem(row + i, rows), half(h), cols(q)]

    def two_up(t):
        return remote(two_piece(t), two_piece(t), up_send.at[t], two_recv.at[t], device(row, z + 1))

    def two_down(t):
        return remote(two_piece(t), two_piece(t), down_send.at[t], two_recv.at[t], device(row, z - 1))

    def feed(q, h):
        t = q * chunk + lax.rem(row - z + rows, rows) * HALVES + h
        return remote(two_held.at[half(h), cols(q)], two_own.at[row, half(h), cols(q)], feed_send.at[q, h],
                      two_recv.at[t], device(z, z))

    def own_two(q, h):
        return pltpu.make_async_copy(two_ref.at[half(h), cols(q)], two_own.at[row, half(h), cols(q)],
                                     two_recv.at[q * chunk + h])

    def feeds(q):
        @pl.when(z != row)
        def _():
            for h in range(HALVES):
                feed(q, h).start()

    def two_swap(q):
        return remote(two_own.at[:, :, cols(q)], two_twin.at[:, :, cols(q)], two_pair.at[0, q], two_pair.at[1, q], twin)

    def one_block(block, h):
        return one.at[core, block, half(h)]

    def one_copy(block, h, target):
        return remote(one_block(block, h), one_block(block, h), one_send.at[block, h, target], one_recv.at[block, h],
                      (target, col))

    def one_swap(block, h):
        return remote(one_block(block, h), one_block(block, h), one_pair.at[0, block, h], one_pair.at[1, block, h],
                      twin)

    def block_of(over, down):
        return lax.rem(b + down, deep) * wide + lax.rem(a + over, wide)

    across = [(over, 0) for over in range(1, wide)]
    along = [(0, down) for down in range(1, deep)]
    far = [(over, down) for over in range(1, wide) for down in range(1, deep)]

    def take_one(block, h):
        arrived(one_block(block, h), one_recv.at[block, h])
        one_swap(block, h).start()

    def weights_swap():
        return remote(pair_ref.at[at(other * width, width)], pair.at[core], weight_sem.at[0], weight_sem.at[1], twin)

    def theirs_swap(q):
        return remote(weighted.at[other, cols(q)], theirs.at[cols(q)], theirs_sem.at[0, q], theirs_sem.at[1, q], twin)

    load_two = pltpu.make_async_copy(two_ref, two_held, load_sem.at[0])
    load_one = pltpu.make_async_copy(one_ref, one.at[core, row], load_sem.at[1])
    load_pair = pltpu.make_async_copy(pair_ref.at[at(core * width, width)], pair.at[core], load_sem.at[2])

    load_two.start()

    @pl.when(home)
    def _():
        for q in range(strips):
            for h in range(HALVES):
                own_two(q, h).start()

    load_one.start()
    load_pair.start()

    barrier = pltpu.get_barrier_semaphore()

    def greet(target):
        pl.semaphore_signal(barrier, inc=1, device_id=target, device_id_type=MESH)

    greet(twin)
    for step in range(1, rows):
        greet((lax.rem(row + step, rows), col))

    @pl.when(z > 0)
    def _():
        greet(device(row, z - 1))

    @pl.when(z < rows - 1)
    def _():
        greet(device(row, z + 1))

    pl.semaphore_wait(barrier, rows + jnp.where(z > 0, 1, 0) + jnp.where(z < rows - 1, 1, 0))
    load_two.wait()
    feeds(0)
    load_one.wait()
    early = [(0, block_of(over, down)) for over, down in across] + [(1, block_of(over, down)) for over, down in along]
    late = [(1, block_of(over, down)) for over, down in across] + [(0, block_of(over, down)) for over, down in along]
    for h, target in early:
        one_copy(row, h, target).start()
    for h, target in late:
        @pl.when(target != z)
        def _(h=h, target=target):
            one_copy(row, h, target).start()
    for h in range(HALVES):
        one_swap(row, h).start()
    weights_swap().start()

    def relays():
        found = []
        for over, down in across:
            for _, other_down in along:
                found.append((block_of(over, down), 0, block_of(0, other_down)))
        for over, down in along:
            for other_over, _ in across:
                found.append((block_of(over, down), 1, block_of(other_over, 0)))
        return found

    def relay_one():
        if strips > 1:
            feeds(1)
        for over, down in across:
            take_one(block_of(over, down), 0)
        for over, down in along:
            take_one(block_of(over, down), 1)
        for block, h, target in relays():
            @pl.when(target != z)
            def _(block=block, h=h, target=target):
                one_copy(block, h, target).start()
        for h, target in late:
            @pl.when(target == z)
            def _(h=h, target=target):
                one_copy(row, h, target).start()
        for block, h, target in relays():
            @pl.when(target == z)
            def _(block=block, h=h, target=target):
                one_copy(block, h, target).start()

    def finish_one():
        for over, down in across:
            take_one(block_of(over, down), 1)
        for over, down in along:
            take_one(block_of(over, down), 0)
        for over, down in far:
            take_one(block_of(over, down), 0)
            take_one(block_of(over, down), 1)
        for block in range(rows):
            for h in range(HALVES):
                arrived(one.at[other, block, half(h)], one_pair.at[1, block, h])
        load_pair.wait()
        arrived(pair.at[other], weight_sem.at[1])

    def correlate(q, p):
        side, i = lax.div(p, tiles), lax.rem(p, tiles)

        @pl.when(p == 0)
        def _():
            turned[...] = two_own[:, :, cols(q)].reshape(rows * samples, strip).T

        columns = at(i * tile, tile)
        total = jnp.dot(turned[...], one[side, :, :, columns].reshape(rows * samples, tile),
                        preferred_element_type=jnp.float32)
        row_ids = (row * CORES + core) * width + q * strip + lax.broadcasted_iota(jnp.int32, total.shape, 0)
        col_ids = (z * CORES + side) * width + i * tile + lax.broadcasted_iota(jnp.int32, total.shape, 1)
        identity = jnp.where(row_ids == col_ids, 1.0, 0.0).astype(jnp.float32)
        scale = pair[side, cols(q), columns].astype(jnp.float32)
        weighted[side, cols(q), columns] = (scale * (total / (rows * samples) - identity)).astype(jnp.bfloat16)

        @pl.when(p == parts - 1)
        def _():
            theirs_swap(q).start()

    def chain_up(g):
        return remote(second_sent.at[g], below.at[g], chain_send.at[g], below_recv.at[g], device(row, z + 1))

    def chain_down(g):
        return remote(second_sent.at[g], above.at[g], chain_send.at[g], above_recv.at[g], device(row, z - 1))

    def spread(g):
        q, i, h = split(g)
        return remote(second_sent.at[g], second_out.at[half(h), cols(q)], spread_send.at[g], spread_recv.at[q, h],
                      device(lax.rem(row + 1 + i, rows), z))

    from_below = jnp.logical_and(z > 0, z <= row)
    from_above = jnp.logical_and(z < rows - 1, z >= row)

    def second_piece(g):
        q, i, h = split(g)
        target = lax.rem(row + 1 + i, rows)
        contract = (((1,), (1,)), ((), ()))
        second_sum[...] = (
            lax.dot_general(one[0, target, half(h)], weighted[0, cols(q)], contract, preferred_element_type=jnp.float32)
            + lax.dot_general(one[1, target, half(h)], weighted[1, cols(q)], contract,
                              preferred_element_type=jnp.float32))

        @pl.when(from_below)
        def _():
            arrived(below.at[g], below_recv.at[g])
            second_sum[...] += below[g].astype(jnp.float32)

        @pl.when(from_above)
        def _():
            arrived(above.at[g], above_recv.at[g])
            second_sum[...] += above[g].astype(jnp.float32)

        keep = jnp.logical_and(home, i == rows - 1)

        second_sent[g] = second_sum[...].astype(jnp.bfloat16)

        @pl.when(keep)
        def _():
            pltpu.make_async_copy(second_sent.at[g], second_out.at[half(h), cols(q)], spread_recv.at[q, h]).start()

        @pl.when(z < row)
        def _():
            chain_up(g).start()

        @pl.when(z > row)
        def _():
            chain_down(g).start()

        @pl.when(jnp.logical_and(home, i != rows - 1))
        def _():
            spread(g).start()

    lead = [(0, over, down) for over, _ in across for down in range(deep)]
    lead_deep = [(1, over, down) for _, down in along for over in range(wide)]
    order = []
    for i in range(max(len(lead), len(lead_deep))):
        order += lead[::-1][i:i + 1] + lead_deep[::-1][i:i + 1]
    opening = len(order)
    order += [(0, 0, down) for _, down in along] + [(1, over, 0) for over, _ in across] + [(0, 0, 0), (1, 0, 0)]

    def unit(u):
        h = pick(u, [entry[0] for entry in order])
        over = pick(u, [entry[1] for entry in order])
        down = pick(u, [entry[2] for entry in order])
        return h, over, down, block_of(over, down)

    def first_hop(u):
        h, over, down, target = unit(u)
        flat = jnp.where(h == 0, (over - 1) * deep + lax.div(target, wide), (down - 1) * wide + lax.rem(target, wide))
        return h, over, down, target, flat

    def wide_open(u):
        h, over, down, target, flat = first_hop(u)
        return remote(first_sent.at[target, half(h)], first_wide.at[flat], first_send.at[u], wide_recv.at[flat],
                      (b * wide + lax.rem(a + over, wide), col))

    def deep_open(u):
        h, over, down, target, flat = first_hop(u)
        return remote(first_sent.at[target, half(h)], first_deep.at[flat], first_send.at[u], deep_recv.at[flat],
                      (lax.rem(b + down, deep) * wide + a, col))

    def deep_close(u):
        h, over, down, target = unit(u)
        return remote(first_sent.at[target, half(h)], deep_sum.at[down - 1], first_send.at[u], deep_last.at[down - 1],
                      (target, col))

    def wide_close(u):
        h, over, down, target = unit(u)
        return remote(first_sent.at[target, half(h)], wide_sum.at[over - 1], first_send.at[u], wide_last.at[over - 1],
                      (target, col))

    def first_tile(target, h, columns):
        return (jnp.dot(two_own[target, half(h)], weighted[core, :, columns], preferred_element_type=jnp.float32)
                + jnp.dot(two_twin[target, half(h)], theirs[:, columns], preferred_element_type=jnp.float32))

    def first_opening(u):
        h, over, down, target = unit(u)

        def body(i, _):
            columns = at(i * tile, tile)
            first_sent[target, half(h), columns] = first_tile(target, h, columns).astype(jnp.bfloat16)
            return 0

        lax.fori_loop(0, tiles, body, 0)

        @pl.when(h == 0)
        def _():
            wide_open(u).start()

        @pl.when(h == 1)
        def _():
            deep_open(u).start()

    def first_closing(u):
        h, over, down, target = unit(u)

        @pl.when(h == 0)
        def _():
            for over_ in range(1, wide):
                flat = (over_ - 1) * deep + lax.div(target, wide)
                arrived(first_wide.at[flat], wide_recv.at[flat])

        @pl.when(h == 1)
        def _():
            for down_ in range(1, deep):
                flat = (down_ - 1) * wide + lax.rem(target, wide)
                arrived(first_deep.at[flat], deep_recv.at[flat])

        def body(i, _):
            columns = at(i * tile, tile)
            total = first_tile(target, h, columns)

            @pl.when(h == 0)
            def _():
                acc = total
                for over_ in range(1, wide):
                    acc += first_wide[(over_ - 1) * deep + lax.div(target, wide), :, columns].astype(jnp.float32)
                first_sent[target, half(h), columns] = acc.astype(jnp.bfloat16)

            @pl.when(h == 1)
            def _():
                acc = total
                for down_ in range(1, deep):
                    acc += first_deep[(down_ - 1) * wide + lax.rem(target, wide), :, columns].astype(jnp.float32)
                first_sent[target, half(h), columns] = acc.astype(jnp.bfloat16)

            return 0

        lax.fori_loop(0, tiles, body, 0)

        @pl.when(h == 0)
        def _():
            deep_close(u).start()

        @pl.when(h == 1)
        def _():
            wide_close(u).start()

    def first_last():
        for _, down in along:
            arrived(deep_sum.at[down - 1], deep_last.at[down - 1])
        for over, _ in across:
            arrived(wide_sum.at[over - 1], wide_last.at[over - 1])
            for d in range(deep):
                @pl.when(d == b)
                def _(over=over, d=d):
                    flat = (over - 1) * deep + d
                    arrived(first_wide.at[flat], wide_recv.at[flat])
        for _, down in along:
            for o in range(wide):
                @pl.when(o == a)
                def _(down=down, o=o):
                    flat = (down - 1) * wide + o
                    arrived(first_deep.at[flat], deep_recv.at[flat])

        def finish_first(i, _):
            columns = at(i * tile, tile)
            top = first_tile(row, 0, columns)
            for over, _ in across:
                top += first_wide[(over - 1) * deep + b, :, columns].astype(jnp.float32)
            for _, down in along:
                top += deep_sum[down - 1, :, columns].astype(jnp.float32)
            first_sent[row, half(0), columns] = top.astype(jnp.bfloat16)
            low = first_tile(row, 1, columns)
            for _, down in along:
                low += first_deep[(down - 1) * wide + a, :, columns].astype(jnp.float32)
            for over, _ in across:
                low += wide_sum[over - 1, :, columns].astype(jnp.float32)
            first_sent[row, half(1), columns] = low.astype(jnp.bfloat16)
            return 0

        lax.fori_loop(0, tiles, finish_first, 0)
        pltpu.make_async_copy(first_sent.at[row], first_out, load_sem.at[3]).start()

    closing = len(order) - 2 - opening
    table = list(range(chunk))
    ends = [chunk - 1]
    for q in range(1, strips):
        if q <= 2:
            owned = [1] if q == 1 else range(2, strips)
            table += [n * chunk + h for n in owned for h in range(HALVES)]
        table += list(range(q * chunk + HALVES, (q + 1) * chunk))
        ends.append(len(table) - 1)
    behind = [max(0, end - (q + 1) * chunk + 1) for q, end in enumerate(ends)]
    shift = max(behind)
    jump = chunk * next((q for q, late_by in enumerate(behind) if late_by), 0)

    soon = back == 1
    def starts(first_lag, later_lag, length):
        found = []
        for q, end in enumerate(ends):
            begin = end + (later_lag if q else first_lag)
            if q + 1 == strips:
                begin = end + (length > 1)
            found.append(max(begin, found[-1] + length) if found else begin)
        return found

    kinds = [starts(0, 0, 1), starts(4, 0, (parts + 1) // 2), starts(6, 2, parts), starts(12, 2, parts)]

    def by_kind(values):
        return jnp.where(last, values[0], jnp.where(soon, values[1], jnp.where(home, values[3], values[2])))

    per = by_kind([parts, 2, 1, 1])
    span = by_kind([1, (parts + 1) // 2, parts, parts])
    second_lag = chunk - 1 + jnp.where(last, 0, 2 + 4 * back)
    second_lag = jnp.where(home, kinds[3][0] + parts, second_lag)
    open_slot = by_kind([kind[-1] for kind in kinds]) + 2
    open_limit = max(kind[-1] for kind in kinds) + 3
    close_slot = open_limit + 8 + jnp.where(home, 5, 0)
    relay_slot = pick(jnp.abs(z - row), [8, 4, 2] + [1] * rows)
    feed_slot = chunk + 2 - jnp.minimum(jnp.abs(z - row), 4)
    slots = pieces + shift + 1 + max(chunk + 1 + 4 * (rows - 1), kinds[3][0] + parts)
    last_slot = jnp.where(home, slots - 5, slots - 1)
    each = (opening + 1) // 2

    def slot(t, _):
        @pl.when(t == relay_slot)
        def _():
            relay_one()

        for q_ in range(2, strips):
            @pl.when(t == feed_slot + (q_ - 1) * (chunk - HALVES))
            def _(q_=q_):
                feeds(q_)

        @pl.when(t < pieces)
        def _():
            n = pick(t, table)
            arrived(two_piece(n), two_recv.at[n])

            @pl.when(jnp.logical_and(z >= row, z < rows - 1))
            def _():
                two_up(n).start()

            @pl.when(jnp.logical_and(z <= row, z > 0))
            def _():
                two_down(n).start()

            @pl.when(lax.rem(n, chunk) == chunk - 1)
            def _():
                two_swap(lax.div(n, chunk)).start()

        @pl.when(t == by_kind([kind[0] for kind in kinds]))
        def _():
            finish_one()

        q, low, high = jnp.int32(0), jnp.int32(0), jnp.int32(0)
        for q_ in range(strips - 1):
            since = t - by_kind([kind[q_] for kind in kinds])
            live = jnp.logical_and(since >= 0, since < span)
            q = jnp.where(live, q_, q)
            low = jnp.where(live, since * per, low)
            high = jnp.where(live, jnp.minimum(since * per + per, parts), high)

        final = t == by_kind([kind[-1] for kind in kinds])
        q = jnp.where(final, strips - 1, q)
        low = jnp.where(final, 0, low)
        high = jnp.where(final, parts, high)

        def piece(i, _):
            correlate(q, i)
            return 0

        lax.fori_loop(low, high, piece, 0)

        @pl.when(t == open_slot)
        def _():
            for q_ in range(strips):
                arrived(two_twin.at[:, :, cols(q_)], two_pair.at[1, q_])
                arrived(theirs.at[cols(q_)], theirs_sem.at[1, q_])

        g = t - second_lag
        g = jnp.where(jnp.logical_or(g < jump, jnp.logical_not(last)), g, jnp.where(g < jump + shift, -1, g - shift))

        @pl.when(jnp.logical_and(g >= 0, g < pieces))
        def _():
            second_piece(g)

        first = jnp.where(t == open_slot, 0, jnp.where(t == open_slot + 1, each, opening))
        final = jnp.where(t == open_slot, each, opening)

        def opener(u, _):
            first_opening(u)
            return 0

        lax.fori_loop(first, final, opener, 0)

        def closer(u, _):
            first_closing(u)
            return 0

        lax.fori_loop(opening, jnp.where(t == close_slot, opening + closing, opening), closer, 0)

        @pl.when(t == last_slot)
        def _():
            first_last()

        return 0

    lax.fori_loop(0, slots, slot, 0)

    for q in range(strips):
        for h in range(HALVES):
            arrived(second_out.at[half(h), cols(q)], spread_recv.at[q, h])

            @pl.when(z != row)
            def _(q=q, h=h):
                feed(q, h).wait_send()

    arrived(first_out, load_sem.at[3])

    def settle(t, _):
        q, i, h = split(t)

        @pl.when(jnp.logical_and(z >= row, z < rows - 1))
        def _():
            two_up(t).wait_send()

        @pl.when(jnp.logical_and(z <= row, z > 0))
        def _():
            two_down(t).wait_send()

        @pl.when(z < row)
        def _():
            chain_up(t).wait_send()

        @pl.when(z > row)
        def _():
            chain_down(t).wait_send()

        @pl.when(jnp.logical_and(home, i != rows - 1))
        def _():
            spread(t).wait_send()

        return 0

    lax.fori_loop(0, pieces, settle, 0)
    for q in range(strips):
        two_swap(q).wait_send()
        theirs_swap(q).wait_send()
    weights_swap().wait_send()
    for h in range(HALVES):
        for over, down in across + along:
            one_copy(row, h, block_of(over, down)).wait_send()
        for block in range(rows):
            one_swap(block, h).wait_send()
    for block, h, target in relays():
        one_copy(block, h, target).wait_send()

    def settle_first(u, _):
        h, over, down, target = unit(u)
        arrived(first_sent.at[target, half(h)], first_send.at[u])
        return 0

    lax.fori_loop(0, opening + closing, settle_first, 0)


def per_device(view_one, view_two, pair_weights):
    rows = lax.axis_size("row")
    samples, width = view_one.shape
    strip = min(width, 256)
    strips = width // strip
    wide, deep = PAIR, rows // PAIR
    part = samples // HALVES
    pieces = strips * rows * HALVES
    units = 2 * rows
    own = jax.ShapeDtypeStruct((samples, width), jnp.bfloat16)
    any_space = pl.BlockSpec(memory_space=pl.ANY)
    dma = pltpu.SemaphoreType.DMA

    def held(*shape):
        return pltpu.VMEM(shape, jnp.bfloat16)

    crossing = (wide - 1) * deep
    descent = (deep - 1) * wide
    return pl.pallas_call(
        lambda *refs: step_kernel(rows, strip, *refs),
        out_shape=(own, own),
        in_specs=[any_space] * 3,
        out_specs=(any_space, any_space),
        scratch_shapes=[
            held(samples, width),
            held(rows, samples, width),
            held(rows, samples, width),
            held(strip, rows * samples),
            held(CORES, rows, samples, width),
            held(CORES, width, width),
            held(CORES, width, width),
            held(width, width),
            held(pieces, part, strip),
            held(pieces, part, strip),
            held(pieces, part, strip),
            pltpu.VMEM((part, strip), jnp.float32),
            held(rows, samples, width),
            held(crossing, part, width),
            held(descent, part, width),
            held(wide - 1, part, width),
            held(deep - 1, part, width),
            dma((4,)),
            dma((pieces,)),
            dma((strips, HALVES)),
            dma((pieces,)),
            dma((pieces,)),
            dma((2, strips)),
            dma((rows, HALVES, rows)),
            dma((rows, HALVES)),
            dma((2, rows, HALVES)),
            dma((2,)),
            dma((2, strips)),
            dma((pieces,)),
            dma((pieces,)),
            dma((pieces,)),
            dma((pieces,)),
            dma((strips, HALVES)),
            dma((units,)),
            dma((crossing,)),
            dma((descent,)),
            dma((wide - 1,)),
            dma((deep - 1,)),
        ],
        compiler_params=pltpu.CompilerParams(collective_id=0, has_side_effects=True, vmem_limit_bytes=62 * 2**20),
        name="twins_step",
    )(view_one, view_two, pair_weights)


def solution(mesh):
    placed = (P("row", "col"), P("row", "col"), P("row", "col"))
    return jax.shard_map(
        per_device,
        mesh=mesh,
        in_specs=placed,
        out_specs=(P("row", "col"), P("row", "col")),
        check_vma=False,
    )
```

```python
import jax
import jax.numpy as jnp
from jax import lax
from jax.experimental import pallas as pl
from jax.experimental.pallas import tpu as pltpu
from jax.sharding import PartitionSpec as P

MESH = pl.DeviceIdType.MESH
CORES = 2
HALVES = 2
PAIR = 2


def arrived(ref, sem):
    pltpu.make_async_copy(ref, ref, sem).wait()


def remote(src, dst, send, recv, device):
    return pltpu.make_async_remote_copy(
        src_ref=src, dst_ref=dst, send_sem=send, recv_sem=recv, device_id=device, device_id_type=MESH
    )


def at(start, size):
    return pl.ds(pl.multiple_of(start, size), size)


def pick(index, values):
    chosen = jnp.int32(values[0])
    for i, value in enumerate(values[1:], 1):
        chosen = jnp.where(index == i, value, chosen)
    return chosen


def step_kernel(rows, strip, one_ref, two_ref, pair_ref, first_out, second_out, two_held, two_own, two_twin, turned, one,
                pair, weighted, theirs, below, above, second_sent, second_sum, first_sent, first_wide, first_deep,
                wide_sum, deep_sum, load_sem, two_recv, feed_send, up_send, down_send, two_pair, one_send, one_recv,
                one_pair, weight_sem, theirs_sem, chain_send, below_recv, above_recv, spread_send, spread_recv,
                first_send, wide_recv, deep_recv, wide_last, deep_last):
    samples, width = two_ref.shape
    wide = PAIR
    deep = rows // wide
    strips = width // strip
    part = samples // HALVES
    chunk = rows * HALVES
    pieces = strips * chunk
    tile = min(width, 512)
    tiles = width // tile
    parts = CORES * tiles
    row, col = lax.axis_index("row"), lax.axis_index("col")
    z, core = lax.div(col, CORES), lax.rem(col, CORES)
    other = 1 - core
    a, b = lax.rem(row, wide), lax.div(row, wide)
    home = z == row
    reach = jnp.where(z > row, rows - 1 - row, jnp.where(z < row, row, jnp.maximum(row, rows - 1 - row)))
    back = reach - jnp.abs(z - row)
    last = back == 0
    back = rows - 1 - jnp.abs(z - row)
    twin = (row, col + 1 - 2 * core)

    def device(target, level):
        return (target, level * CORES + core)

    def half(h):
        return at(h * part, part)

    def cols(q):
        return at(q * strip, strip)

    def split(t):
        return lax.div(t, chunk), lax.rem(lax.div(t, HALVES), rows), lax.rem(t, HALVES)

    across = [(over, 0) for over in range(1, wide)]
    along = [(0, down) for down in range(1, deep)]
    far = [(over, down) for over in range(1, wide) for down in range(1, deep)]
    sources = [(0, 0)] + along + far + across
    targets = far + across + along + [(0, 0)]

    def block_of(over, down):
        return lax.rem(b + down, deep) * wide + lax.rem(a + over, wide)

    def choose(i, pairs):
        return block_of(pick(i, [over for over, _ in pairs]), pick(i, [down for _, down in pairs]))

    def two_piece(t):
        q, i, h = split(t)
        return two_own.at[choose(i, sources), half(h), cols(q)]

    def two_up(t):
        return remote(two_piece(t), two_piece(t), up_send.at[t], two_recv.at[t], device(row, z + 1))

    def two_down(t):
        return remote(two_piece(t), two_piece(t), down_send.at[t], two_recv.at[t], device(row, z - 1))

    def feed(q, h):
        over = lax.rem(a - lax.rem(z, wide) + wide, wide)
        down = lax.rem(b - lax.div(z, wide) + deep, deep)
        place = pick(over * deep + down, [sources.index((o, d)) for o in range(wide) for d in range(deep)])
        t = q * chunk + place * HALVES + h
        return remote(two_held.at[half(h), cols(q)], two_own.at[row, half(h), cols(q)], feed_send.at[q, h],
                      two_recv.at[t], device(z, z))

    def own_two(q, h):
        return pltpu.make_async_copy(two_ref.at[half(h), cols(q)], two_own.at[row, half(h), cols(q)],
                                     two_recv.at[q * chunk + h])

    def feeds(q):
        @pl.when(z != row)
        def _():
            for h in range(HALVES):
                feed(q, h).start()

    def two_swap(q):
        return remote(two_own.at[:, :, cols(q)], two_twin.at[:, :, cols(q)], two_pair.at[0, q], two_pair.at[1, q], twin)

    def one_block(block, h):
        return one.at[core, block, half(h)]

    def one_copy(block, h, target):
        return remote(one_block(block, h), one_block(block, h), one_send.at[block, h, target], one_recv.at[block, h],
                      (target, col))

    def one_swap(block, h):
        return remote(one_block(block, h), one_block(block, h), one_pair.at[0, block, h], one_pair.at[1, block, h],
                      twin)

    def take_one(block, h):
        arrived(one_block(block, h), one_recv.at[block, h])
        one_swap(block, h).start()

    def weights_swap():
        return remote(pair_ref.at[at(other * width, width)], pair.at[core], weight_sem.at[0], weight_sem.at[1], twin)

    def theirs_swap(q):
        return remote(weighted.at[other, cols(q)], theirs.at[cols(q)], theirs_sem.at[0, q], theirs_sem.at[1, q], twin)

    load_two = pltpu.make_async_copy(two_ref, two_held, load_sem.at[0])
    load_one = pltpu.make_async_copy(one_ref, one.at[core, row], load_sem.at[1])
    load_pair = pltpu.make_async_copy(pair_ref.at[at(core * width, width)], pair.at[core], load_sem.at[2])

    load_two.start()

    @pl.when(home)
    def _():
        for q in range(strips):
            for h in range(HALVES):
                own_two(q, h).start()

    load_one.start()
    load_pair.start()

    barrier = pltpu.get_barrier_semaphore()

    def greet(target):
        pl.semaphore_signal(barrier, inc=1, device_id=target, device_id_type=MESH)

    greet(twin)
    for step in range(1, rows):
        greet((lax.rem(row + step, rows), col))

    @pl.when(z > 0)
    def _():
        greet(device(row, z - 1))

    @pl.when(z < rows - 1)
    def _():
        greet(device(row, z + 1))

    pl.semaphore_wait(barrier, rows + jnp.where(z > 0, 1, 0) + jnp.where(z < rows - 1, 1, 0))
    load_two.wait()
    feeds(0)
    load_one.wait()
    early = [(0, block_of(over, down)) for over, down in across] + [(1, block_of(over, down)) for over, down in along]
    late = [(1, block_of(over, down)) for over, down in across] + [(0, block_of(over, down)) for over, down in along]
    for h, target in early:
        one_copy(row, h, target).start()
    for h, target in late:
        @pl.when(target != z)
        def _(h=h, target=target):
            one_copy(row, h, target).start()
    for h in range(HALVES):
        one_swap(row, h).start()
    weights_swap().start()

    def relays():
        found = []
        for over, down in across:
            for _, other_down in along:
                target = block_of(0, other_down)
                found.append((block_of(over, down), 0, target, target != z))
        for over, down in along:
            for other_over, _ in across:
                target = block_of(other_over, 0)
                found.append((block_of(over, down), 1, target, True))
        return found

    def late_relays():
        found = []
        for over, down in along:
            for other_over, _ in across:
                target = block_of(other_over, 0)
                found.append((block_of(over, down), 0, target, target == z))
        return found

    def relay_one():
        if strips > 1:
            feeds(1)
        for over, down in across:
            take_one(block_of(over, down), 0)
        for over, down in along:
            take_one(block_of(over, down), 1)
        for block, h, target, live in relays():
            @pl.when(jnp.logical_and(live, target != z))
            def _(block=block, h=h, target=target):
                one_copy(block, h, target).start()
        for h, target in late:
            @pl.when(target == z)
            def _(h=h, target=target):
                one_copy(row, h, target).start()
        for block, h, target, live in relays():
            @pl.when(jnp.logical_and(live, target == z))
            def _(block=block, h=h, target=target):
                one_copy(block, h, target).start()

    def finish_one():
        for over, down in across:
            take_one(block_of(over, down), 1)
        for over, down in along:
            take_one(block_of(over, down), 0)
        for block, h, target, live in late_relays():
            @pl.when(live)
            def _(block=block, h=h, target=target):
                one_copy(block, h, target).start()
        for over, down in far:
            take_one(block_of(over, down), 0)
            take_one(block_of(over, down), 1)
        for block in range(rows):
            for h in range(HALVES):
                arrived(one.at[other, block, half(h)], one_pair.at[1, block, h])
        load_pair.wait()
        arrived(pair.at[other], weight_sem.at[1])

    def correlate(q, p):
        side, i = lax.div(p, tiles), lax.rem(p, tiles)

        @pl.when(p == 0)
        def _():
            turned[...] = two_own[:, :, cols(q)].reshape(rows * samples, strip).T

        columns = at(i * tile, tile)
        total = jnp.dot(turned[...], one[side, :, :, columns].reshape(rows * samples, tile),
                        preferred_element_type=jnp.float32)
        row_ids = (row * CORES + core) * width + q * strip + lax.broadcasted_iota(jnp.int32, total.shape, 0)
        col_ids = (z * CORES + side) * width + i * tile + lax.broadcasted_iota(jnp.int32, total.shape, 1)
        identity = jnp.where(row_ids == col_ids, 1.0, 0.0).astype(jnp.float32)
        scale = pair[side, cols(q), columns].astype(jnp.float32)
        weighted[side, cols(q), columns] = (scale * (total / (rows * samples) - identity)).astype(jnp.bfloat16)

        @pl.when(p == parts - 1)
        def _():
            theirs_swap(q).start()

    def chain_up(g):
        return remote(second_sent.at[g], below.at[g], chain_send.at[g], below_recv.at[g], device(row, z + 1))

    def chain_down(g):
        return remote(second_sent.at[g], above.at[g], chain_send.at[g], above_recv.at[g], device(row, z - 1))

    def spread(g):
        q, i, h = split(g)
        return remote(second_sent.at[g], second_out.at[half(h), cols(q)], spread_send.at[g], spread_recv.at[q, h],
                      device(choose(i, targets), z))

    from_below = jnp.logical_and(z > 0, z <= row)
    from_above = jnp.logical_and(z < rows - 1, z >= row)

    def second_piece(g):
        q, i, h = split(g)
        target = choose(i, targets)
        contract = (((1,), (1,)), ((), ()))
        second_sum[...] = (
            lax.dot_general(one[0, target, half(h)], weighted[0, cols(q)], contract, preferred_element_type=jnp.float32)
            + lax.dot_general(one[1, target, half(h)], weighted[1, cols(q)], contract,
                              preferred_element_type=jnp.float32))

        @pl.when(from_below)
        def _():
            arrived(below.at[g], below_recv.at[g])
            second_sum[...] += below[g].astype(jnp.float32)

        @pl.when(from_above)
        def _():
            arrived(above.at[g], above_recv.at[g])
            second_sum[...] += above[g].astype(jnp.float32)

        keep = jnp.logical_and(home, i == rows - 1)

        second_sent[g] = second_sum[...].astype(jnp.bfloat16)

        @pl.when(keep)
        def _():
            pltpu.make_async_copy(second_sent.at[g], second_out.at[half(h), cols(q)], spread_recv.at[q, h]).start()

        @pl.when(z < row)
        def _():
            chain_up(g).start()

        @pl.when(z > row)
        def _():
            chain_down(g).start()

        @pl.when(jnp.logical_and(home, i != rows - 1))
        def _():
            spread(g).start()

    lead = [(0, over, down) for over, _ in across for down in range(deep)]
    lead_deep = [(1, over, down) for _, down in along for over in range(wide)]
    order = []
    for i in range(max(len(lead), len(lead_deep))):
        order += lead[::-1][i:i + 1] + lead_deep[::-1][i:i + 1]
    opening = len(order)
    order += [(0, 0, down) for _, down in along] + [(1, over, 0) for over, _ in across] + [(0, 0, 0), (1, 0, 0)]

    def unit(u):
        h = pick(u, [entry[0] for entry in order])
        over = pick(u, [entry[1] for entry in order])
        down = pick(u, [entry[2] for entry in order])
        return h, over, down, block_of(over, down)

    def first_hop(u):
        h, over, down, target = unit(u)
        flat = jnp.where(h == 0, (over - 1) * deep + lax.div(target, wide), (down - 1) * wide + lax.rem(target, wide))
        return h, over, down, target, flat

    def wide_open(u):
        h, over, down, target, flat = first_hop(u)
        return remote(first_sent.at[target, half(h)], first_wide.at[flat], first_send.at[u], wide_recv.at[flat],
                      (b * wide + lax.rem(a + over, wide), col))

    def deep_open(u):
        h, over, down, target, flat = first_hop(u)
        return remote(first_sent.at[target, half(h)], first_deep.at[flat], first_send.at[u], deep_recv.at[flat],
                      (lax.rem(b + down, deep) * wide + a, col))

    def deep_close(u):
        h, over, down, target = unit(u)
        return remote(first_sent.at[target, half(h)], deep_sum.at[down - 1], first_send.at[u], deep_last.at[down - 1],
                      (target, col))

    def wide_close(u):
        h, over, down, target = unit(u)
        return remote(first_sent.at[target, half(h)], wide_sum.at[over - 1], first_send.at[u], wide_last.at[over - 1],
                      (target, col))

    def first_tile(target, h, columns):
        return (jnp.dot(two_own[target, half(h)], weighted[core, :, columns], preferred_element_type=jnp.float32)
                + jnp.dot(two_twin[target, half(h)], theirs[:, columns], preferred_element_type=jnp.float32))

    def first_opening(u):
        h, over, down, target = unit(u)

        def body(i, _):
            columns = at(i * tile, tile)
            first_sent[target, half(h), columns] = first_tile(target, h, columns).astype(jnp.bfloat16)
            return 0

        lax.fori_loop(0, tiles, body, 0)

        @pl.when(h == 0)
        def _():
            wide_open(u).start()

        @pl.when(h == 1)
        def _():
            deep_open(u).start()

    def first_closing(u):
        h, over, down, target = unit(u)

        @pl.when(h == 0)
        def _():
            for over_ in range(1, wide):
                flat = (over_ - 1) * deep + lax.div(target, wide)
                arrived(first_wide.at[flat], wide_recv.at[flat])

        @pl.when(h == 1)
        def _():
            for down_ in range(1, deep):
                flat = (down_ - 1) * wide + lax.rem(target, wide)
                arrived(first_deep.at[flat], deep_recv.at[flat])

        def body(i, _):
            columns = at(i * tile, tile)
            total = first_tile(target, h, columns)

            @pl.when(h == 0)
            def _():
                acc = total
                for over_ in range(1, wide):
                    acc += first_wide[(over_ - 1) * deep + lax.div(target, wide), :, columns].astype(jnp.float32)
                first_sent[target, half(h), columns] = acc.astype(jnp.bfloat16)

            @pl.when(h == 1)
            def _():
                acc = total
                for down_ in range(1, deep):
                    acc += first_deep[(down_ - 1) * wide + lax.rem(target, wide), :, columns].astype(jnp.float32)
                first_sent[target, half(h), columns] = acc.astype(jnp.bfloat16)

            return 0

        lax.fori_loop(0, tiles, body, 0)

        @pl.when(h == 0)
        def _():
            deep_close(u).start()

        @pl.when(h == 1)
        def _():
            wide_close(u).start()

    def first_last():
        for _, down in along:
            arrived(deep_sum.at[down - 1], deep_last.at[down - 1])
        for over, _ in across:
            arrived(wide_sum.at[over - 1], wide_last.at[over - 1])
            for d in range(deep):
                @pl.when(d == b)
                def _(over=over, d=d):
                    flat = (over - 1) * deep + d
                    arrived(first_wide.at[flat], wide_recv.at[flat])
        for _, down in along:
            for o in range(wide):
                @pl.when(o == a)
                def _(down=down, o=o):
                    flat = (down - 1) * wide + o
                    arrived(first_deep.at[flat], deep_recv.at[flat])

        def finish_first(i, _):
            columns = at(i * tile, tile)
            top = first_tile(row, 0, columns)
            for over, _ in across:
                top += first_wide[(over - 1) * deep + b, :, columns].astype(jnp.float32)
            for _, down in along:
                top += deep_sum[down - 1, :, columns].astype(jnp.float32)
            first_sent[row, half(0), columns] = top.astype(jnp.bfloat16)
            low = first_tile(row, 1, columns)
            for _, down in along:
                low += first_deep[(down - 1) * wide + a, :, columns].astype(jnp.float32)
            for over, _ in across:
                low += wide_sum[over - 1, :, columns].astype(jnp.float32)
            first_sent[row, half(1), columns] = low.astype(jnp.bfloat16)
            return 0

        lax.fori_loop(0, tiles, finish_first, 0)
        pltpu.make_async_copy(first_sent.at[row], first_out, load_sem.at[3]).start()

    closing = len(order) - 2 - opening
    def run(q, order):
        return [q * chunk + sources.index(pair) * HALVES + h for pair in order for h in range(HALVES)]

    table = run(0, [(0, 0)] + across + along + far)
    ends = [chunk - 1]
    for q in range(1, strips):
        if q <= 2:
            for owned in [1] if q == 1 else range(2, strips):
                table += run(owned, [(0, 0)])
        table += run(q, sources[1:])
        ends.append(len(table) - 1)
    shift = max(end - (q + 1) * chunk + 1 for q, end in enumerate(ends))
    soon = jnp.logical_and(back == 1, jnp.logical_not(last))
    def starts(first_lag, later_lag, length):
        found = []
        for q, end in enumerate(ends):
            begin = end + (later_lag if q else first_lag)
            if q + 1 == strips:
                begin = end + (length > 1)
            found.append(max(begin, found[-1] + length) if found else begin)
        return found

    kinds = [starts(0, 0, 1), starts(4, 0, (parts + 1) // 2), starts(6, 2, parts), starts(13, 2, parts)]

    def by_kind(values):
        return jnp.where(last, values[0], jnp.where(soon, values[1], jnp.where(home, values[3], values[2])))

    per = by_kind([parts, 2, 1, 1])
    span = by_kind([1, (parts + 1) // 2, parts, parts])
    home_lag = max(kinds[3][0] + parts, chunk + 1 + 4 * (rows - 1))
    second_lag = jnp.where(last, chunk - 1, jnp.where(home, home_lag, chunk + 1 + 4 * back))
    second_slot = by_kind([kind[0] for kind in kinds]) + jnp.where(last, 0, span)
    open_slot = by_kind([kind[-1] for kind in kinds]) + 2
    open_limit = max(kind[-1] for kind in kinds) + 3
    close_slot = open_limit + by_kind([6, 6, 8, 12])
    relay_slot = pick(jnp.abs(z - row), [8, 4, 2] + [1] * rows)
    feed_slot = chunk + 1 - jnp.minimum(jnp.abs(z - row), 4)
    slots = pieces + 1 + home_lag + shift
    last_slot = slots - 1
    each = (opening + 1) // 2

    def slot(t, _):
        @pl.when(t == relay_slot)
        def _():
            relay_one()

        for q_ in range(2, strips):
            @pl.when(t == feed_slot + (q_ - 2) * (chunk - HALVES))
            def _(q_=q_):
                feeds(q_)

        @pl.when(t < pieces)
        def _():
            n = pick(t, table)
            arrived(two_piece(n), two_recv.at[n])

            @pl.when(jnp.logical_and(z >= row, z < rows - 1))
            def _():
                two_up(n).start()

            @pl.when(jnp.logical_and(z <= row, z > 0))
            def _():
                two_down(n).start()

            for q_ in range(strips):
                @pl.when(t == ends[q_])
                def _(q_=q_):
                    two_swap(q_).start()

        @pl.when(t == by_kind([kind[0] for kind in kinds]))
        def _():
            finish_one()

        q, low, high = jnp.int32(0), jnp.int32(0), jnp.int32(0)
        for q_ in range(strips - 1):
            since = t - by_kind([kind[q_] for kind in kinds])
            live = jnp.logical_and(since >= 0, since < span)
            q = jnp.where(live, q_, q)
            low = jnp.where(live, since * per, low)
            high = jnp.where(live, jnp.minimum(since * per + per, parts), high)

        final = t == by_kind([kind[-1] for kind in kinds])
        q = jnp.where(final, strips - 1, q)
        low = jnp.where(final, 0, low)
        high = jnp.where(final, parts, high)

        def piece(i, _):
            correlate(q, i)
            return 0

        lax.fori_loop(low, high, piece, 0)

        @pl.when(t == open_slot)
        def _():
            for q_ in range(strips):
                arrived(two_twin.at[:, :, cols(q_)], two_pair.at[1, q_])
                arrived(theirs.at[cols(q_)], theirs_sem.at[1, q_])

        def second_count(t):
            ahead = t - second_lag + 1
            count = jnp.maximum(jnp.minimum(ahead, 2 * chunk), ahead - shift)
            count = jnp.maximum(count, jnp.where(soon, jnp.minimum(ahead + 2, chunk), 0))
            return jnp.where(t < second_slot, 0, jnp.clip(count, 0, pieces))

        def second(g, _):
            second_piece(g)
            return 0

        lax.fori_loop(second_count(t - 1), second_count(t), second, 0)

        first = jnp.where(t == open_slot, 0, jnp.where(t == open_slot + 1, each, opening))
        final = jnp.where(t == open_slot, each, opening)

        def opener(u, _):
            first_opening(u)
            return 0

        lax.fori_loop(first, final, opener, 0)

        def closer(u, _):
            first_closing(u)
            return 0

        lax.fori_loop(opening, jnp.where(t == close_slot, opening + closing, opening), closer, 0)

        @pl.when(t == last_slot)
        def _():
            first_last()

        return 0

    lax.fori_loop(0, slots, slot, 0)

    for q in range(strips):
        for h in range(HALVES):
            arrived(second_out.at[half(h), cols(q)], spread_recv.at[q, h])

            @pl.when(z != row)
            def _(q=q, h=h):
                feed(q, h).wait_send()

    arrived(first_out, load_sem.at[3])

    def settle(t, _):
        q, i, h = split(t)

        @pl.when(jnp.logical_and(z >= row, z < rows - 1))
        def _():
            two_up(t).wait_send()

        @pl.when(jnp.logical_and(z <= row, z > 0))
        def _():
            two_down(t).wait_send()

        @pl.when(z < row)
        def _():
            chain_up(t).wait_send()

        @pl.when(z > row)
        def _():
            chain_down(t).wait_send()

        @pl.when(jnp.logical_and(home, i != rows - 1))
        def _():
            spread(t).wait_send()

        return 0

    lax.fori_loop(0, pieces, settle, 0)
    for q in range(strips):
        two_swap(q).wait_send()
        theirs_swap(q).wait_send()
    weights_swap().wait_send()
    for h in range(HALVES):
        for over, down in across + along:
            one_copy(row, h, block_of(over, down)).wait_send()
        for block in range(rows):
            one_swap(block, h).wait_send()
    for block, h, target, live in relays() + late_relays():
        @pl.when(live)
        def _(block=block, h=h, target=target):
            one_copy(block, h, target).wait_send()

    def settle_first(u, _):
        h, over, down, target = unit(u)
        arrived(first_sent.at[target, half(h)], first_send.at[u])
        return 0

    lax.fori_loop(0, opening + closing, settle_first, 0)


def per_device(view_one, view_two, pair_weights):
    rows = lax.axis_size("row")
    samples, width = view_one.shape
    strip = min(width, 256)
    strips = width // strip
    wide, deep = PAIR, rows // PAIR
    part = samples // HALVES
    pieces = strips * rows * HALVES
    units = 2 * rows
    own = jax.ShapeDtypeStruct((samples, width), jnp.bfloat16)
    any_space = pl.BlockSpec(memory_space=pl.ANY)
    dma = pltpu.SemaphoreType.DMA

    def held(*shape):
        return pltpu.VMEM(shape, jnp.bfloat16)

    crossing = (wide - 1) * deep
    descent = (deep - 1) * wide
    return pl.pallas_call(
        lambda *refs: step_kernel(rows, strip, *refs),
        out_shape=(own, own),
        in_specs=[any_space] * 3,
        out_specs=(any_space, any_space),
        scratch_shapes=[
            held(samples, width),
            held(rows, samples, width),
            held(rows, samples, width),
            held(strip, rows * samples),
            held(CORES, rows, samples, width),
            held(CORES, width, width),
            held(CORES, width, width),
            held(width, width),
            held(pieces, part, strip),
            held(pieces, part, strip),
            held(pieces, part, strip),
            pltpu.VMEM((part, strip), jnp.float32),
            held(rows, samples, width),
            held(crossing, part, width),
            held(descent, part, width),
            held(wide - 1, part, width),
            held(deep - 1, part, width),
            dma((4,)),
            dma((pieces,)),
            dma((strips, HALVES)),
            dma((pieces,)),
            dma((pieces,)),
            dma((2, strips)),
            dma((rows, HALVES, rows)),
            dma((rows, HALVES)),
            dma((2, rows, HALVES)),
            dma((2,)),
            dma((2, strips)),
            dma((pieces,)),
            dma((pieces,)),
            dma((pieces,)),
            dma((pieces,)),
            dma((strips, HALVES)),
            dma((units,)),
            dma((crossing,)),
            dma((descent,)),
            dma((wide - 1,)),
            dma((deep - 1,)),
        ],
        compiler_params=pltpu.CompilerParams(collective_id=0, has_side_effects=True, vmem_limit_bytes=62 * 2**20),
        name="twins_step",
    )(view_one, view_two, pair_weights)


def solution(mesh):
    placed = (P("row", "col"), P("row", "col"), P("row", "col"))
    return jax.shard_map(
        per_device,
        mesh=mesh,
        in_specs=placed,
        out_specs=(P("row", "col"), P("row", "col")),
        check_vma=False,
    )
```

```python
import jax
import jax.numpy as jnp
from jax import lax
from jax.experimental import pallas as pl
from jax.experimental.pallas import tpu as pltpu
from jax.sharding import PartitionSpec as P

MESH = pl.DeviceIdType.MESH
CORES = 2
HALVES = 2
QUARTERS = 4
PAIR = 2


def arrived(ref, sem):
    pltpu.make_async_copy(ref, ref, sem).wait()


def remote(src, dst, send, recv, device):
    return pltpu.make_async_remote_copy(
        src_ref=src, dst_ref=dst, send_sem=send, recv_sem=recv, device_id=device, device_id_type=MESH
    )


def at(start, size):
    return pl.ds(pl.multiple_of(start, size), size)


def pick(index, values):
    chosen = jnp.int32(values[0])
    for i, value in enumerate(values[1:], 1):
        chosen = jnp.where(index == i, value, chosen)
    return chosen


def step_kernel(rows, strip, one_ref, two_ref, pair_ref, first_out, second_out, two_held, two_own, two_twin, turned, one,
                pair, weighted, theirs, below, above, second_sent, second_sum, first_sent, first_wide, first_deep,
                wide_sum, deep_sum, first_own, load_sem, two_recv, one_send, one_recv, below_recv, above_recv, wide_recv,
                deep_recv, wide_last, deep_last, sent, whole):
    samples, width = two_ref.shape
    wide = PAIR
    deep = rows // wide
    strips = width // strip
    part = samples // HALVES
    chunk = rows * HALVES
    pieces = strips * chunk
    tile = min(width, 512)
    tiles = width // tile
    parts = CORES * tiles
    row, col = lax.axis_index("row"), lax.axis_index("col")
    z, core = lax.div(col, CORES), lax.rem(col, CORES)
    other = 1 - core
    a, b = lax.rem(row, wide), lax.div(row, wide)
    home = z == row
    reach = jnp.where(z > row, rows - 1 - row, jnp.where(z < row, row, jnp.maximum(row, rows - 1 - row)))
    back = reach - jnp.abs(z - row)
    last = back == 0
    back = rows - 1 - jnp.abs(z - row)
    twin = (row, col + 1 - 2 * core)

    def device(target, level):
        return (target, level * CORES + core)

    def half(h):
        return at(h * part, part)

    def cols(q):
        return at(q * strip, strip)

    def split(t):
        return lax.div(t, chunk), lax.rem(lax.div(t, HALVES), rows), lax.rem(t, HALVES)

    across = [(over, 0) for over in range(1, wide)]
    along = [(0, down) for down in range(1, deep)]
    far = [(over, down) for over in range(1, wide) for down in range(1, deep)]
    sources = [(0, 0)] + along + far + across
    targets = far + across + along + [(0, 0)]

    def block_of(over, down):
        return lax.rem(b + down, deep) * wide + lax.rem(a + over, wide)

    def choose(i, pairs):
        return block_of(pick(i, [over for over, _ in pairs]), pick(i, [down for _, down in pairs]))

    def two_piece(t):
        q, i, h = split(t)
        return two_own.at[choose(i, sources), half(h), cols(q)]

    def two_up(t):
        return remote(two_piece(t), two_piece(t), sent.at[0], two_recv.at[t], device(row, z + 1))

    def two_down(t):
        return remote(two_piece(t), two_piece(t), sent.at[1], two_recv.at[t], device(row, z - 1))

    def feed(q, h):
        over = lax.rem(a - lax.rem(z, wide) + wide, wide)
        down = lax.rem(b - lax.div(z, wide) + deep, deep)
        place = pick(over * deep + down, [sources.index((o, d)) for o in range(wide) for d in range(deep)])
        t = q * chunk + place * HALVES + h
        return remote(two_held.at[half(h), cols(q)], two_own.at[row, half(h), cols(q)], sent.at[2],
                      two_recv.at[t], device(z, z))

    def own_two(q, h):
        return pltpu.make_async_copy(two_ref.at[half(h), cols(q)], two_own.at[row, half(h), cols(q)],
                                     two_recv.at[q * chunk + h])

    def feeds(q):
        @pl.when(z != row)
        def _():
            for h in range(HALVES):
                feed(q, h).start()

    def two_swap(q):
        return remote(two_own.at[:, :, cols(q)], two_twin.at[:, :, cols(q)], sent.at[3], whole.at[0], twin)

    def one_block(block, h):
        return one.at[core, block, half(h)]

    def one_copy(block, h, target, send):
        return remote(one_block(block, h), one_block(block, h), send, one_recv.at[block, h], (target, col))

    def one_swap(block, h):
        return remote(one_block(block, h), one_block(block, h), sent.at[4], whole.at[1], twin)

    def take_one(block, h):
        arrived(one_block(block, h), one_recv.at[block, h])
        one_swap(block, h).start()

    def weights_swap():
        return remote(pair_ref.at[at(other * width, width)], pair.at[core], sent.at[6], whole.at[3], twin)

    def theirs_swap(q):
        return remote(weighted.at[other, cols(q)], theirs.at[cols(q)], sent.at[5], whole.at[2], twin)

    load_two = pltpu.make_async_copy(two_ref, two_held, load_sem.at[0])
    load_one = pltpu.make_async_copy(one_ref, one.at[core, row], load_sem.at[1])
    load_pair = pltpu.make_async_copy(pair_ref.at[at(core * width, width)], pair.at[core], load_sem.at[2])

    load_two.start()

    @pl.when(home)
    def _():
        for q in range(strips):
            for h in range(HALVES):
                own_two(q, h).start()

    load_one.start()
    load_pair.start()

    barrier = pltpu.get_barrier_semaphore()

    def greet(target):
        pl.semaphore_signal(barrier, inc=1, device_id=target, device_id_type=MESH)

    greet(twin)
    for step in range(1, rows):
        greet((lax.rem(row + step, rows), col))

    @pl.when(z > 0)
    def _():
        greet(device(row, z - 1))

    @pl.when(z < rows - 1)
    def _():
        greet(device(row, z + 1))

    pl.semaphore_wait(barrier, rows + jnp.where(z > 0, 1, 0) + jnp.where(z < rows - 1, 1, 0))
    load_two.wait()
    feeds(0)
    load_one.wait()
    early = [(0, block_of(over, down)) for over, down in across] + [(1, block_of(over, down)) for over, down in along]
    late = [(1, block_of(over, down)) for over, down in across] + [(0, block_of(over, down)) for over, down in along]
    for h, target in early:
        one_copy(row, h, target, sent.at[7]).start()
    for h, target in late:
        @pl.when(target != z)
        def _(h=h, target=target):
            one_copy(row, h, target, sent.at[7]).start()
    for h in range(HALVES):
        one_swap(row, h).start()
    weights_swap().start()

    def relays():
        found = []
        for over, down in across:
            for i, (_, other_down) in enumerate(along):
                target = block_of(0, other_down)
                found.append((block_of(over, down), 0, target, target != z, i))
        for over, down in along:
            for i, (other_over, _) in enumerate(across):
                target = block_of(other_over, 0)
                found.append((block_of(over, down), 1, target, True, i))
        return found

    def late_relays():
        found = []
        for over, down in along:
            for i, (other_over, _) in enumerate(across):
                target = block_of(other_over, 0)
                found.append((block_of(over, down), 0, target, target == z, i))
        return found

    def relay(block, h, target, i):
        return one_copy(block, h, target, one_send.at[block, h, i])

    def relay_one():
        if strips > 1:
            feeds(1)
        for over, down in across:
            take_one(block_of(over, down), 0)
        for over, down in along:
            take_one(block_of(over, down), 1)
        for block, h, target, live, i in relays():
            @pl.when(jnp.logical_and(live, target != z))
            def _(block=block, h=h, target=target, i=i):
                relay(block, h, target, i).start()
        for h, target in late:
            @pl.when(target == z)
            def _(h=h, target=target):
                one_copy(row, h, target, sent.at[7]).start()
        for block, h, target, live, i in relays():
            @pl.when(jnp.logical_and(live, target == z))
            def _(block=block, h=h, target=target, i=i):
                relay(block, h, target, i).start()

    def finish_one():
        for over, down in across:
            take_one(block_of(over, down), 1)
        for over, down in along:
            take_one(block_of(over, down), 0)
        for block, h, target, live, i in late_relays():
            @pl.when(live)
            def _(block=block, h=h, target=target, i=i):
                relay(block, h, target, i).start()
        for over, down in far:
            take_one(block_of(over, down), 0)
            take_one(block_of(over, down), 1)
        arrived(one.at[other], whole.at[1])
        load_pair.wait()
        arrived(pair.at[other], whole.at[3])

    def correlate(q, p):
        side, i = lax.div(p, tiles), lax.rem(p, tiles)

        @pl.when(p == 0)
        def _():
            turned[...] = two_own[:, :, cols(q)].reshape(rows * samples, strip).T

        columns = at(i * tile, tile)
        total = jnp.dot(turned[...], one[side, :, :, columns].reshape(rows * samples, tile),
                        preferred_element_type=jnp.float32)
        row_ids = (row * CORES + core) * width + q * strip + lax.broadcasted_iota(jnp.int32, total.shape, 0)
        col_ids = (z * CORES + side) * width + i * tile + lax.broadcasted_iota(jnp.int32, total.shape, 1)
        identity = jnp.where(row_ids == col_ids, 1.0, 0.0).astype(jnp.float32)
        scale = pair[side, cols(q), columns].astype(jnp.float32)
        weighted[side, cols(q), columns] = (scale * (total / (rows * samples) - identity)).astype(jnp.bfloat16)

        @pl.when(p == parts - 1)
        def _():
            theirs_swap(q).start()

    def chain_up(g):
        return remote(second_sent.at[g], below.at[g], sent.at[8], below_recv.at[g], device(row, z + 1))

    def chain_down(g):
        return remote(second_sent.at[g], above.at[g], sent.at[8], above_recv.at[g], device(row, z - 1))

    def spread(g):
        q, i, h = split(g)
        return remote(second_sent.at[g], second_out.at[half(h), cols(q)], sent.at[9], whole.at[4],
                      device(choose(i, targets), z))

    from_below = jnp.logical_and(z > 0, z <= row)
    from_above = jnp.logical_and(z < rows - 1, z >= row)

    def second_piece(g):
        q, i, h = split(g)
        target = choose(i, targets)
        contract = (((1,), (1,)), ((), ()))
        second_sum[...] = (
            lax.dot_general(one[0, target, half(h)], weighted[0, cols(q)], contract, preferred_element_type=jnp.float32)
            + lax.dot_general(one[1, target, half(h)], weighted[1, cols(q)], contract,
                              preferred_element_type=jnp.float32))

        @pl.when(from_below)
        def _():
            arrived(below.at[g], below_recv.at[g])
            second_sum[...] += below[g].astype(jnp.float32)

        @pl.when(from_above)
        def _():
            arrived(above.at[g], above_recv.at[g])
            second_sum[...] += above[g].astype(jnp.float32)

        keep = jnp.logical_and(home, i == rows - 1)

        second_sent[g] = second_sum[...].astype(jnp.bfloat16)

        @pl.when(keep)
        def _():
            pltpu.make_async_copy(second_sent.at[g], second_out.at[half(h), cols(q)], whole.at[4]).start()

        @pl.when(z < row)
        def _():
            chain_up(g).start()

        @pl.when(z > row)
        def _():
            chain_down(g).start()

        @pl.when(jnp.logical_and(home, i != rows - 1))
        def _():
            spread(g).start()

    lead = [(0, over, down) for over, _ in across for down in range(deep)]
    lead_deep = [(1, over, down) for _, down in along for over in range(wide)]
    order = []
    for i in range(max(len(lead), len(lead_deep))):
        order += lead[::-1][i:i + 1] + lead_deep[::-1][i:i + 1]
    opening = len(order)
    order += [(0, 0, down) for _, down in along] + [(1, over, 0) for over, _ in across] + [(0, 0, 0), (1, 0, 0)]

    def unit(u):
        h = pick(u, [entry[0] for entry in order])
        over = pick(u, [entry[1] for entry in order])
        down = pick(u, [entry[2] for entry in order])
        return h, over, down, block_of(over, down)

    def first_hop(u):
        h, over, down, target = unit(u)
        flat = jnp.where(h == 0, (over - 1) * deep + lax.div(target, wide), (down - 1) * wide + lax.rem(target, wide))
        return h, over, down, target, flat

    def wide_open(u):
        h, over, down, target, flat = first_hop(u)
        return remote(first_sent.at[target, half(h)], first_wide.at[flat], sent.at[10], wide_recv.at[flat],
                      (b * wide + lax.rem(a + over, wide), col))

    def deep_open(u):
        h, over, down, target, flat = first_hop(u)
        return remote(first_sent.at[target, half(h)], first_deep.at[flat], sent.at[10], deep_recv.at[flat],
                      (lax.rem(b + down, deep) * wide + a, col))

    def deep_close(u):
        h, over, down, target = unit(u)
        return remote(first_sent.at[target, half(h)], deep_sum.at[down - 1], sent.at[10], deep_last.at[down - 1],
                      (target, col))

    def wide_close(u):
        h, over, down, target = unit(u)
        return remote(first_sent.at[target, half(h)], wide_sum.at[over - 1], sent.at[10], wide_last.at[over - 1],
                      (target, col))

    def first_tile(target, h, columns):
        return (jnp.dot(two_own[target, half(h)], weighted[core, :, columns], preferred_element_type=jnp.float32)
                + jnp.dot(two_twin[target, half(h)], theirs[:, columns], preferred_element_type=jnp.float32))

    def first_opening(u):
        h, over, down, target = unit(u)

        def body(i, _):
            columns = at(i * tile, tile)
            first_sent[target, half(h), columns] = first_tile(target, h, columns).astype(jnp.bfloat16)
            return 0

        lax.fori_loop(0, tiles, body, 0)

        @pl.when(h == 0)
        def _():
            wide_open(u).start()

        @pl.when(h == 1)
        def _():
            deep_open(u).start()

    def first_closing(u):
        h, over, down, target = unit(u)

        @pl.when(h == 0)
        def _():
            for over_ in range(1, wide):
                flat = (over_ - 1) * deep + lax.div(target, wide)
                arrived(first_wide.at[flat], wide_recv.at[flat])

        @pl.when(h == 1)
        def _():
            for down_ in range(1, deep):
                flat = (down_ - 1) * wide + lax.rem(target, wide)
                arrived(first_deep.at[flat], deep_recv.at[flat])

        def body(i, _):
            columns = at(i * tile, tile)
            total = first_tile(target, h, columns)

            @pl.when(h == 0)
            def _():
                acc = total
                for over_ in range(1, wide):
                    acc += first_wide[(over_ - 1) * deep + lax.div(target, wide), :, columns].astype(jnp.float32)
                first_sent[target, half(h), columns] = acc.astype(jnp.bfloat16)

            @pl.when(h == 1)
            def _():
                acc = total
                for down_ in range(1, deep):
                    acc += first_deep[(down_ - 1) * wide + lax.rem(target, wide), :, columns].astype(jnp.float32)
                first_sent[target, half(h), columns] = acc.astype(jnp.bfloat16)

            return 0

        lax.fori_loop(0, tiles, body, 0)

        @pl.when(h == 0)
        def _():
            deep_close(u).start()

        @pl.when(h == 1)
        def _():
            wide_close(u).start()

    def first_last():
        for _, down in along:
            arrived(deep_sum.at[down - 1], deep_last.at[down - 1])
        for over, _ in across:
            arrived(wide_sum.at[over - 1], wide_last.at[over - 1])
            for d in range(deep):
                @pl.when(d == b)
                def _(over=over, d=d):
                    flat = (over - 1) * deep + d
                    arrived(first_wide.at[flat], wide_recv.at[flat])
        for _, down in along:
            for o in range(wide):
                @pl.when(o == a)
                def _(down=down, o=o):
                    flat = (down - 1) * wide + o
                    arrived(first_deep.at[flat], deep_recv.at[flat])

        def finish_first(i, _):
            columns = at(i * tile, tile)
            top = first_own[half(0), columns]
            for over, _ in across:
                top += first_wide[(over - 1) * deep + b, :, columns].astype(jnp.float32)
            for _, down in along:
                top += deep_sum[down - 1, :, columns].astype(jnp.float32)
            first_sent[row, half(0), columns] = top.astype(jnp.bfloat16)
            low = first_own[half(1), columns]
            for _, down in along:
                low += first_deep[(down - 1) * wide + a, :, columns].astype(jnp.float32)
            for over, _ in across:
                low += wide_sum[over - 1, :, columns].astype(jnp.float32)
            first_sent[row, half(1), columns] = low.astype(jnp.bfloat16)
            return 0

        lax.fori_loop(0, tiles, finish_first, 0)
        pltpu.make_async_copy(first_sent.at[row], first_out, load_sem.at[3]).start()

    closing = len(order) - 2 - opening
    def run(q, order):
        return [q * chunk + sources.index(pair) * HALVES + h for pair in order for h in range(HALVES)]

    table = run(0, [(0, 0)] + across + along + far)
    ends = [chunk - 1]
    for q in range(1, strips):
        if q <= 2:
            for owned in [1] if q == 1 else range(2, strips):
                table += run(owned, [(0, 0)])
        table += run(q, sources[1:])
        ends.append(len(table) - 1)
    shift = max(end - (q + 1) * chunk + 1 for q, end in enumerate(ends))
    soon = jnp.logical_and(back == 1, jnp.logical_not(last))
    def starts(first_lag, later_lag, length):
        found = []
        for q, end in enumerate(ends):
            begin = end + (later_lag if q else first_lag)
            if q + 1 == strips:
                begin = end + (length > 1)
            found.append(max(begin, found[-1] + length) if found else begin)
        return found

    kinds = [starts(0, 0, 1), starts(4, 0, (parts + 1) // 2), starts(6, 2, parts), starts(13, 2, parts)]

    def by_kind(values):
        return jnp.where(last, values[0], jnp.where(soon, values[1], jnp.where(home, values[3], values[2])))

    per = by_kind([parts, 2, 1, 1])
    span = by_kind([1, (parts + 1) // 2, parts, parts])
    home_lag = max(kinds[3][0] + parts, chunk + 1 + 4 * (rows - 1))
    second_lag = jnp.where(last, chunk - 1, jnp.where(home, home_lag, chunk + 1 + 4 * back))
    second_slot = by_kind([kind[0] for kind in kinds]) + jnp.where(last, 0, span)
    open_slot = by_kind([kind[-1] for kind in kinds]) + 2
    open_limit = max(kind[-1] for kind in kinds) + 1 + opening
    close_slot = open_limit + by_kind([6, 6, 8, 12])
    relay_slot = pick(jnp.abs(z - row), [8, 4, 2] + [1] * rows)
    feed_slot = chunk + 1 - jnp.minimum(jnp.abs(z - row), 4)
    slots = pieces + 1 + home_lag + shift
    last_slot = slots - 1
    each = (opening + 1) // 2

    def slot(t, _):
        @pl.when(t == relay_slot)
        def _():
            relay_one()

        for q_ in range(2, strips):
            @pl.when(t == feed_slot + (q_ - 2) * (chunk - HALVES))
            def _(q_=q_):
                feeds(q_)

        @pl.when(t < pieces)
        def _():
            n = pick(t, table)
            arrived(two_piece(n), two_recv.at[n])

            @pl.when(jnp.logical_and(z >= row, z < rows - 1))
            def _():
                two_up(n).start()

            @pl.when(jnp.logical_and(z <= row, z > 0))
            def _():
                two_down(n).start()

            for q_ in range(strips):
                @pl.when(t == ends[q_])
                def _(q_=q_):
                    two_swap(q_).start()

        @pl.when(t == by_kind([kind[0] for kind in kinds]))
        def _():
            finish_one()

        q, low, high = jnp.int32(0), jnp.int32(0), jnp.int32(0)
        for q_ in range(strips - 1):
            since = t - by_kind([kind[q_] for kind in kinds])
            live = jnp.logical_and(since >= 0, since < span)
            q = jnp.where(live, q_, q)
            low = jnp.where(live, since * per, low)
            high = jnp.where(live, jnp.minimum(since * per + per, parts), high)

        final = t == by_kind([kind[-1] for kind in kinds])
        q = jnp.where(final, strips - 1, q)
        low = jnp.where(final, 0, low)
        high = jnp.where(final, parts, high)

        def piece(i, _):
            correlate(q, i)
            return 0

        lax.fori_loop(low, high, piece, 0)

        @pl.when(t == open_slot)
        def _():
            arrived(two_twin, whole.at[0])
            arrived(theirs, whole.at[2])

        def second_count(t):
            ahead = t - second_lag + 1
            count = jnp.maximum(jnp.minimum(ahead, 2 * chunk), ahead - shift)
            count = jnp.maximum(count, jnp.where(soon, jnp.minimum(ahead + 2, chunk), 0))
            return jnp.where(t < second_slot, 0, jnp.clip(count, 0, pieces))

        def second(g, _):
            second_piece(g)
            return 0

        lax.fori_loop(second_count(t - 1), second_count(t), second, 0)

        turn = t - open_slot
        first = jnp.where(turn > 0, turn + 1, 0)
        final = jnp.where(jnp.logical_and(turn >= 0, turn < opening - 1), turn + 2, first)

        def opener(u, _):
            first_opening(u)
            return 0

        lax.fori_loop(first, final, opener, 0)

        def closer(u, _):
            first_closing(u)
            return 0

        turn = t - close_slot
        first = opening + turn
        final = jnp.where(jnp.logical_and(turn >= 0, turn < closing), first + 1, first)
        lax.fori_loop(first, final, closer, 0)
        turn = t - open_slot - opening

        @pl.when(jnp.logical_and(turn >= 0, turn < HALVES * tiles))
        def _():
            h, columns = lax.div(turn, tiles), at(lax.rem(turn, tiles) * tile, tile)
            first_own[half(h), columns] = first_tile(row, h, columns)

        @pl.when(t == last_slot)
        def _():
            first_last()

        return 0

    lax.fori_loop(0, slots, slot, 0)

    arrived(second_out, whole.at[4])
    arrived(first_out, load_sem.at[3])

    @pl.when(z != row)
    def _():
        arrived(two_held, sent.at[2])
        arrived(second_sent, sent.at[8])

    @pl.when(home)
    def _():
        arrived(second_sent.at[pl.ds(0, pieces - strips * HALVES)], sent.at[9])

    @pl.when(jnp.logical_and(z >= row, z < rows - 1))
    def _():
        arrived(two_own, sent.at[0])

    @pl.when(jnp.logical_and(z <= row, z > 0))
    def _():
        arrived(two_own, sent.at[1])

    arrived(two_own, sent.at[3])
    arrived(one.at[core], sent.at[4])
    arrived(weighted.at[other], sent.at[5])
    arrived(pair.at[core], sent.at[6])
    arrived(one.at[core, pl.ds(0, len(across + along))], sent.at[7])
    for block, h, target, live, i in relays() + late_relays():
        @pl.when(live)
        def _(block=block, h=h, target=target, i=i):
            relay(block, h, target, i).wait_send()

    arrived(first_sent.at[pl.ds(0, rows - 1)], sent.at[10])


def settle_kernel(first_ref, second_ref, first_out, second_out, first, second, load, store):
    pairs = ((first_ref, first, first_out), (second_ref, second, second_out))
    part = first_ref.shape[0] // QUARTERS

    def copy(which, i, out):
        source, held, target = pairs[which]
        here = pl.ds(i * part, part)
        if out:
            return pltpu.make_async_copy(held.at[here], target.at[here], store.at[which, i])
        return pltpu.make_async_copy(source.at[here], held.at[here], load.at[which, i])

    order = [(which, i) for i in range(QUARTERS) for which in range(2)]
    for which, i in order:
        copy(which, i, False).start()
    for which, i in order:
        copy(which, i, False).wait()
        copy(which, i, True).start()
    for which, i in order:
        copy(which, i, True).wait()


def settle(first, second):
    any_space = pl.BlockSpec(memory_space=pl.ANY)
    dma = pltpu.SemaphoreType.DMA
    return pl.pallas_call(
        settle_kernel,
        out_shape=[jax.ShapeDtypeStruct(x.shape, x.dtype) for x in (first, second)],
        in_specs=[any_space] * 2,
        out_specs=[any_space] * 2,
        scratch_shapes=[pltpu.VMEM(x.shape, x.dtype) for x in (first, second)] + [dma((2, QUARTERS))] * 2,
        name="settle_grads",
    )(first, second)


def per_device(view_one, view_two, pair_weights):
    rows = lax.axis_size("row")
    samples, width = view_one.shape
    strip = min(width, 256)
    strips = width // strip
    wide, deep = PAIR, rows // PAIR
    part = samples // HALVES
    pieces = strips * rows * HALVES
    own = jax.ShapeDtypeStruct((samples, width), jnp.bfloat16)
    any_space = pl.BlockSpec(memory_space=pl.ANY)
    dma = pltpu.SemaphoreType.DMA

    def held(*shape):
        return pltpu.VMEM(shape, jnp.bfloat16)

    crossing = (wide - 1) * deep
    descent = (deep - 1) * wide
    first, second = pl.pallas_call(
        lambda *refs: step_kernel(rows, strip, *refs),
        out_shape=(own, own),
        in_specs=[any_space] * 3,
        out_specs=(any_space, any_space),
        scratch_shapes=[
            held(samples, width),
            held(rows, samples, width),
            held(rows, samples, width),
            held(strip, rows * samples),
            held(CORES, rows, samples, width),
            held(CORES, width, width),
            held(CORES, width, width),
            held(width, width),
            held(pieces, part, strip),
            held(pieces, part, strip),
            held(pieces, part, strip),
            pltpu.VMEM((part, strip), jnp.float32),
            held(rows, samples, width),
            held(crossing, part, width),
            held(descent, part, width),
            held(wide - 1, part, width),
            held(deep - 1, part, width),
            pltpu.VMEM((samples, width), jnp.float32),
            dma((4,)),
            dma((pieces,)),
            dma((rows, HALVES, max(wide, deep) - 1)),
            dma((rows, HALVES)),
            dma((pieces,)),
            dma((pieces,)),
            dma((crossing,)),
            dma((descent,)),
            dma((wide - 1,)),
            dma((deep - 1,)),
            dma((11,)),
            dma((5,)),
        ],
        compiler_params=pltpu.CompilerParams(collective_id=0, has_side_effects=True, vmem_limit_bytes=62 * 2**20),
        name="twins_step",
    )(view_one, view_two, pair_weights)
    return settle(first, second)


def solution(mesh):
    placed = (P("row", "col"), P("row", "col"), P("row", "col"))
    return jax.shard_map(
        per_device,
        mesh=mesh,
        in_specs=placed,
        out_specs=(P("row", "col"), P("row", "col")),
        check_vma=False,
    )
```

```python
import jax
import jax.numpy as jnp
from jax import lax
from jax.experimental import pallas as pl
from jax.experimental.pallas import tpu as pltpu
from jax.sharding import PartitionSpec as P

MESH = pl.DeviceIdType.MESH
CORES = 2
HALVES = 2
QUARTERS = 4
PAIR = 2


def arrived(ref, sem):
    pltpu.make_async_copy(ref, ref, sem).wait()


def remote(src, dst, send, recv, device):
    return pltpu.make_async_remote_copy(
        src_ref=src, dst_ref=dst, send_sem=send, recv_sem=recv, device_id=device, device_id_type=MESH
    )


def at(start, size):
    return pl.ds(pl.multiple_of(start, size), size)


def pick(index, values):
    chosen = jnp.int32(values[0])
    for i, value in enumerate(values[1:], 1):
        chosen = jnp.where(index == i, value, chosen)
    return chosen


def step_kernel(rows, strip, one_ref, two_ref, pair_ref, first_out, second_out, two_held, two_own, two_twin, turned, one,
                pair, weighted, theirs, below, above, second_sent, second_sum, first_sent, first_wide, first_deep,
                wide_sum, deep_sum, first_own, passing, handed, load_sem, two_recv, one_send, one_recv, below_recv, above_recv, wide_recv,
                deep_recv, wide_last, deep_last, pass_recv, handed_recv, sent, whole):
    samples, width = two_ref.shape
    wide = PAIR
    deep = rows // wide
    strips = width // strip
    part = samples // HALVES
    chunk = rows * HALVES
    pieces = strips * chunk
    tile = min(width, 512)
    tiles = width // tile
    parts = CORES * tiles
    row, col = lax.axis_index("row"), lax.axis_index("col")
    z, core = lax.div(col, CORES), lax.rem(col, CORES)
    other = 1 - core
    a, b = lax.rem(row, wide), lax.div(row, wide)
    home = z == row
    reach = jnp.where(z > row, rows - 1 - row, jnp.where(z < row, row, jnp.maximum(row, rows - 1 - row)))
    back = reach - jnp.abs(z - row)
    last = back == 0
    back = rows - 1 - jnp.abs(z - row)
    twin = (row, col + 1 - 2 * core)

    def device(target, level):
        return (target, level * CORES + core)

    def half(h):
        return at(h * part, part)

    def cols(q):
        return at(q * strip, strip)

    def split(t):
        return lax.div(t, chunk), lax.rem(lax.div(t, HALVES), rows), lax.rem(t, HALVES)

    across = [(over, 0) for over in range(1, wide)]
    along = [(0, down) for down in range(1, deep)]
    far = [(over, down) for over in range(1, wide) for down in range(1, deep)]
    sources = [(0, 0)] + across + along + far
    targets = far + across + along + [(0, 0)]

    def block_of(over, down):
        return lax.rem(b + down, deep) * wide + lax.rem(a + over, wide)

    def choose(i, pairs):
        return block_of(pick(i, [over for over, _ in pairs]), pick(i, [down for _, down in pairs]))

    def two_piece(t):
        q, i, h = split(t)
        return two_own.at[choose(i, sources), half(h), cols(q)]

    def two_up(t):
        return remote(two_piece(t), two_piece(t), sent.at[0], two_recv.at[t], device(row, z + 1))

    def two_down(t):
        return remote(two_piece(t), two_piece(t), sent.at[1], two_recv.at[t], device(row, z - 1))

    def feed(q, h):
        over = lax.rem(a - lax.rem(z, wide) + wide, wide)
        down = lax.rem(b - lax.div(z, wide) + deep, deep)
        place = pick(over * deep + down, [sources.index((o, d)) for o in range(wide) for d in range(deep)])
        t = q * chunk + place * HALVES + h
        return remote(two_held.at[half(h), cols(q)], two_own.at[row, half(h), cols(q)], sent.at[2],
                      two_recv.at[t], device(z, z))

    def own_two(q, h):
        return pltpu.make_async_copy(two_ref.at[half(h), cols(q)], two_own.at[row, half(h), cols(q)],
                                     two_recv.at[q * chunk + h])

    home_a, home_b = lax.rem(z, wide), lax.div(z, wide)
    remote_a, remote_b = a != home_a, b != home_b

    home_a, home_b = lax.rem(z, wide), lax.div(z, wide)
    remote_a, remote_b = a != home_a, b != home_b
    opposite = jnp.logical_and(remote_a, remote_b)
    helper = jnp.logical_and(remote_a, jnp.logical_not(remote_b))
    detours = list(range(0, strips, 2))

    def hand(q, h):
        place = lax.rem(b - home_b + deep, deep) - 1
        n = detours.index(q)
        return remote(two_held.at[half(h), cols(q)], handed.at[n, place, half(h)], sent.at[2],
                      handed_recv.at[n, place, h], device(home_b * wide + a, z))

    def hand_on(q, down, h):
        over = lax.rem(a - home_a + wide, wide)
        place = pick(over, [sources.index((max(o, 1), down)) for o in range(wide)])
        n = detours.index(q)
        return remote(handed.at[n, down - 1, half(h)], two_own.at[block_of(0, down), half(h), cols(q)], sent.at[12],
                      two_recv.at[q * chunk + place * HALVES + h], device(z, z))

    def hand_over(q):
        for _, down in along:
            for h in range(HALVES):
                arrived(handed.at[detours.index(q), down - 1, half(h)], handed_recv.at[detours.index(q), down - 1, h])
                hand_on(q, down, h).start()

    def feeds(q):
        direct = jnp.logical_and(z != row, jnp.logical_not(opposite)) if q in detours else z != row

        @pl.when(direct)
        def _():
            for h in range(HALVES):
                feed(q, h).start()

        if q in detours:
            @pl.when(opposite)
            def _():
                for h in range(HALVES):
                    hand(q, h).start()

    def two_swap(q):
        return remote(two_own.at[:, :, cols(q)], two_twin.at[:, :, cols(q)], sent.at[3], whole.at[0], twin)

    def one_block(block, h):
        return one.at[core, block, half(h)]

    def one_copy(block, h, target, send):
        return remote(one_block(block, h), one_block(block, h), send, one_recv.at[block, h], (target, col))

    def one_swap(block, h):
        return remote(one_block(block, h), one_block(block, h), sent.at[4], whole.at[1], twin)

    def take_one(block, h):
        arrived(one_block(block, h), one_recv.at[block, h])
        one_swap(block, h).start()

    def weights_swap():
        return remote(pair_ref.at[at(other * width, width)], pair.at[core], sent.at[6], whole.at[3], twin)

    def theirs_swap(q):
        return remote(weighted.at[other, cols(q)], theirs.at[cols(q)], sent.at[5], whole.at[2], twin)

    load_two = pltpu.make_async_copy(two_ref, two_held, load_sem.at[0])
    load_one = pltpu.make_async_copy(one_ref, one.at[core, row], load_sem.at[1])
    load_pair = pltpu.make_async_copy(pair_ref.at[at(core * width, width)], pair.at[core], load_sem.at[2])

    load_two.start()

    @pl.when(home)
    def _():
        for q in range(strips):
            for h in range(HALVES):
                own_two(q, h).start()

    load_one.start()
    load_pair.start()

    barrier = pltpu.get_barrier_semaphore()

    def greet(target):
        pl.semaphore_signal(barrier, inc=1, device_id=target, device_id_type=MESH)

    greet(twin)
    for step in range(1, rows):
        greet((lax.rem(row + step, rows), col))

    @pl.when(z > 0)
    def _():
        greet(device(row, z - 1))

    @pl.when(z < rows - 1)
    def _():
        greet(device(row, z + 1))

    pl.semaphore_wait(barrier, rows + jnp.where(z > 0, 1, 0) + jnp.where(z < rows - 1, 1, 0))
    load_two.wait()

    feeds(0)
    load_one.wait()
    early = [(0, block_of(over, down)) for over, down in across] + [(1, block_of(over, down)) for over, down in along]
    late = [(1, block_of(over, down)) for over, down in across] + [(0, block_of(over, down)) for over, down in along]
    for h, target in early + late:
        @pl.when(target != z)
        def _(h=h, target=target):
            one_copy(row, h, target, sent.at[7]).start()
    for h in range(HALVES):
        one_swap(row, h).start()
    weights_swap().start()

    @pl.when(helper)
    def _():
        hand_over(0)

    for h, target in early:
        @pl.when(target == z)
        def _(h=h, target=target):
            one_copy(row, h, target, sent.at[7]).start()

    def relays():
        found = []
        for over, down in across:
            for i, (_, other_down) in enumerate(along):
                target = block_of(0, other_down)
                found.append((block_of(over, down), 0, target, i))
        for over, down in along:
            for i, (other_over, _) in enumerate(across):
                target = block_of(other_over, 0)
                found.append((block_of(over, down), 1, target, i))
        return found

    def relay(block, h, target, i):
        return one_copy(block, h, target, one_send.at[block, h, i])

    def relay_one():
        if strips > 1:
            feeds(1)
        for over, down in across:
            take_one(block_of(over, down), 0)
        for over, down in along:
            take_one(block_of(over, down), 1)
        for block, h, target, i in relays():
            @pl.when(target != z)
            def _(block=block, h=h, target=target, i=i):
                relay(block, h, target, i).start()
        for h, target in late:
            @pl.when(target == z)
            def _(h=h, target=target):
                one_copy(row, h, target, sent.at[7]).start()
        for block, h, target, i in relays():
            @pl.when(target == z)
            def _(block=block, h=h, target=target, i=i):
                relay(block, h, target, i).start()

    def finish_one():
        for over, down in across:
            take_one(block_of(over, down), 1)
        for over, down in along:
            take_one(block_of(over, down), 0)
        for over, down in far:
            take_one(block_of(over, down), 0)
            take_one(block_of(over, down), 1)
        arrived(one.at[other], whole.at[1])
        load_pair.wait()
        arrived(pair.at[other], whole.at[3])

    def correlate(q, p):
        side, i = lax.div(p, tiles), lax.rem(p, tiles)

        @pl.when(p == 0)
        def _():
            turned[...] = two_own[:, :, cols(q)].reshape(rows * samples, strip).T

        columns = at(i * tile, tile)
        total = jnp.dot(turned[...], one[side, :, :, columns].reshape(rows * samples, tile),
                        preferred_element_type=jnp.float32)
        row_ids = (row * CORES + core) * width + q * strip + lax.broadcasted_iota(jnp.int32, total.shape, 0)
        col_ids = (z * CORES + side) * width + i * tile + lax.broadcasted_iota(jnp.int32, total.shape, 1)
        identity = jnp.where(row_ids == col_ids, 1.0, 0.0).astype(jnp.float32)
        scale = pair[side, cols(q), columns].astype(jnp.float32)
        weighted[side, cols(q), columns] = (scale * (total / (rows * samples) - identity)).astype(jnp.bfloat16)

        @pl.when(p == parts - 1)
        def _():
            theirs_swap(q).start()

    def chain_up(g):
        return remote(second_sent.at[g], below.at[g], sent.at[8], below_recv.at[g], device(row, z + 1))

    def chain_down(g):
        return remote(second_sent.at[g], above.at[g], sent.at[8], above_recv.at[g], device(row, z - 1))

    def spread(g):
        q, i, h = split(g)
        return remote(second_sent.at[g], second_out.at[half(h), cols(q)], sent.at[9], whole.at[4],
                      device(choose(i, targets), z))

    def via(g):
        q, i, h = split(g)
        return remote(second_sent.at[g], passing.at[q, pick(i, [over for over, _ in targets]) - 1], sent.at[9],
                      pass_recv.at[q, pick(i, [over for over, _ in targets]) - 1],
                      device(block_of(0, pick(i, [down for _, down in targets])), z))

    def pass_on(q, over):
        return remote(passing.at[q, over - 1], second_out.at[half(HALVES - 1), cols(q)], sent.at[11], whole.at[4],
                      device(block_of(over, 0), z))

    middle = jnp.logical_and(a == lax.rem(z, wide), b != lax.div(z, wide))

    from_below = jnp.logical_and(z > 0, z <= row)
    from_above = jnp.logical_and(z < rows - 1, z >= row)

    def second_piece(g):
        q, i, h = split(g)
        target = choose(i, targets)
        contract = (((1,), (1,)), ((), ()))
        second_sum[...] = (
            lax.dot_general(one[0, target, half(h)], weighted[0, cols(q)], contract, preferred_element_type=jnp.float32)
            + lax.dot_general(one[1, target, half(h)], weighted[1, cols(q)], contract,
                              preferred_element_type=jnp.float32))

        @pl.when(from_below)
        def _():
            arrived(below.at[g], below_recv.at[g])
            second_sum[...] += below[g].astype(jnp.float32)

        @pl.when(from_above)
        def _():
            arrived(above.at[g], above_recv.at[g])
            second_sum[...] += above[g].astype(jnp.float32)

        keep = jnp.logical_and(home, i == rows - 1)

        second_sent[g] = second_sum[...].astype(jnp.bfloat16)

        @pl.when(keep)
        def _():
            pltpu.make_async_copy(second_sent.at[g], second_out.at[half(h), cols(q)], whole.at[4]).start()

        @pl.when(z < row)
        def _():
            chain_up(g).start()

        @pl.when(z > row)
        def _():
            chain_down(g).start()

        turned_off = jnp.logical_and(h == HALVES - 1, i < len(far))

        @pl.when(jnp.logical_and(home, turned_off))
        def _():
            via(g).start()

        @pl.when(jnp.logical_and(home, jnp.logical_not(jnp.logical_or(turned_off, i == rows - 1))))
        def _():
            spread(g).start()

    lead = [(0, over, down) for over, _ in across for down in range(deep)]
    lead_deep = [(1, over, down) for _, down in along for over in range(wide)]
    order = []
    for i in range(max(len(lead), len(lead_deep))):
        order += lead[::-1][i:i + 1] + lead_deep[::-1][i:i + 1]
    opening = len(order)
    order += [(0, 0, down) for _, down in along] + [(1, over, 0) for over, _ in across] + [(0, 0, 0), (1, 0, 0)]

    def unit(u):
        h = pick(u, [entry[0] for entry in order])
        over = pick(u, [entry[1] for entry in order])
        down = pick(u, [entry[2] for entry in order])
        return h, over, down, block_of(over, down)

    def first_hop(u):
        h, over, down, target = unit(u)
        flat = jnp.where(h == 0, (over - 1) * deep + lax.div(target, wide), (down - 1) * wide + lax.rem(target, wide))
        return h, over, down, target, flat

    def wide_open(u):
        h, over, down, target, flat = first_hop(u)
        return remote(first_sent.at[target, half(h)], first_wide.at[flat], sent.at[10], wide_recv.at[flat],
                      (b * wide + lax.rem(a + over, wide), col))

    def deep_open(u):
        h, over, down, target, flat = first_hop(u)
        return remote(first_sent.at[target, half(h)], first_deep.at[flat], sent.at[10], deep_recv.at[flat],
                      (lax.rem(b + down, deep) * wide + a, col))

    def deep_close(u):
        h, over, down, target = unit(u)
        return remote(first_sent.at[target, half(h)], deep_sum.at[down - 1], sent.at[10], deep_last.at[down - 1],
                      (target, col))

    def wide_close(u):
        h, over, down, target = unit(u)
        return remote(first_sent.at[target, half(h)], wide_sum.at[over - 1], sent.at[10], wide_last.at[over - 1],
                      (target, col))

    def first_tile(target, h, columns):
        return (jnp.dot(two_own[target, half(h)], weighted[core, :, columns], preferred_element_type=jnp.float32)
                + jnp.dot(two_twin[target, half(h)], theirs[:, columns], preferred_element_type=jnp.float32))

    def first_opening(u):
        h, over, down, target = unit(u)

        def body(i, _):
            columns = at(i * tile, tile)
            first_sent[target, half(h), columns] = first_tile(target, h, columns).astype(jnp.bfloat16)
            return 0

        lax.fori_loop(0, tiles, body, 0)

        @pl.when(h == 0)
        def _():
            wide_open(u).start()

        @pl.when(h == 1)
        def _():
            deep_open(u).start()

    def first_closing(u):
        h, over, down, target = unit(u)

        @pl.when(h == 0)
        def _():
            for over_ in range(1, wide):
                flat = (over_ - 1) * deep + lax.div(target, wide)
                arrived(first_wide.at[flat], wide_recv.at[flat])

        @pl.when(h == 1)
        def _():
            for down_ in range(1, deep):
                flat = (down_ - 1) * wide + lax.rem(target, wide)
                arrived(first_deep.at[flat], deep_recv.at[flat])

        def body(i, _):
            columns = at(i * tile, tile)
            total = first_tile(target, h, columns)

            @pl.when(h == 0)
            def _():
                acc = total
                for over_ in range(1, wide):
                    acc += first_wide[(over_ - 1) * deep + lax.div(target, wide), :, columns].astype(jnp.float32)
                first_sent[target, half(h), columns] = acc.astype(jnp.bfloat16)

            @pl.when(h == 1)
            def _():
                acc = total
                for down_ in range(1, deep):
                    acc += first_deep[(down_ - 1) * wide + lax.rem(target, wide), :, columns].astype(jnp.float32)
                first_sent[target, half(h), columns] = acc.astype(jnp.bfloat16)

            return 0

        lax.fori_loop(0, tiles, body, 0)

        @pl.when(h == 0)
        def _():
            deep_close(u).start()

        @pl.when(h == 1)
        def _():
            wide_close(u).start()

    def first_last():
        for _, down in along:
            arrived(deep_sum.at[down - 1], deep_last.at[down - 1])
        for over, _ in across:
            arrived(wide_sum.at[over - 1], wide_last.at[over - 1])
            for d in range(deep):
                @pl.when(d == b)
                def _(over=over, d=d):
                    flat = (over - 1) * deep + d
                    arrived(first_wide.at[flat], wide_recv.at[flat])
        for _, down in along:
            for o in range(wide):
                @pl.when(o == a)
                def _(down=down, o=o):
                    flat = (down - 1) * wide + o
                    arrived(first_deep.at[flat], deep_recv.at[flat])

        def finish_first(i, _):
            columns = at(i * tile, tile)
            top = first_own[half(0), columns]
            for over, _ in across:
                top += first_wide[(over - 1) * deep + b, :, columns].astype(jnp.float32)
            for _, down in along:
                top += deep_sum[down - 1, :, columns].astype(jnp.float32)
            first_sent[row, half(0), columns] = top.astype(jnp.bfloat16)
            low = first_own[half(1), columns]
            for _, down in along:
                low += first_deep[(down - 1) * wide + a, :, columns].astype(jnp.float32)
            for over, _ in across:
                low += wide_sum[over - 1, :, columns].astype(jnp.float32)
            first_sent[row, half(1), columns] = low.astype(jnp.bfloat16)
            return 0

        lax.fori_loop(0, tiles, finish_first, 0)
        pltpu.make_async_copy(first_sent.at[row], first_out, load_sem.at[3]).start()

    closing = len(order) - 2 - opening
    def run(q, order):
        return [q * chunk + sources.index(pair) * HALVES + h for pair in order for h in range(HALVES)]

    table = run(0, sources)
    ends = [chunk - 1]
    for q in range(1, strips):
        if q <= 2:
            for owned in [1] if q == 1 else range(2, strips):
                table += run(owned, [(0, 0)])
        table += run(q, sources[1:])
        ends.append(len(table) - 1)
    shift = max(end - (q + 1) * chunk + 1 for q, end in enumerate(ends))
    soon = jnp.logical_and(back == 1, jnp.logical_not(last))
    def starts(first_lag, later_lag, length):
        found = []
        for q, end in enumerate(ends):
            begin = end + (later_lag if q else first_lag)
            if q + 1 == strips:
                begin = end + (length > 1)
            found.append(max(begin, found[-1] + length) if found else begin)
        return found

    kinds = [starts(0, 0, 1), starts(4, 0, (parts + 1) // 2), starts(6, 2, (parts + 1) // 2), starts(14, 2, 1)]

    def by_kind(values):
        return jnp.where(last, values[0], jnp.where(soon, values[1], jnp.where(home, values[3], values[2])))

    per = by_kind([parts, 2, 2, parts])
    span = by_kind([1, (parts + 1) // 2, (parts + 1) // 2, 1])
    home_lag = max(kinds[3][0] + 2, chunk + 4 * (rows - 1))
    second_lag = jnp.where(last, chunk - 1, jnp.where(home, home_lag, chunk + 4 * back))
    second_slot = by_kind([kind[0] for kind in kinds]) + jnp.where(jnp.logical_or(last, home), 0, span)
    open_slot = by_kind([kind[-1] for kind in kinds]) + 2
    open_limit = max(kind[-1] for kind in kinds) + 1 + opening
    close_slot = open_limit + by_kind([6, 6, 8, 11])
    relay_slot = pick(jnp.abs(z - row), [8, 4, 2] + [1] * rows)
    feed_slot = chunk + 1 - jnp.minimum(jnp.abs(z - row), 4)
    slots = pieces + 1 + home_lag + shift
    last_slot = slots - 1
    each = (opening + 1) // 2

    def slot(t, _):
        @pl.when(t == relay_slot)
        def _():
            relay_one()

        for q_ in range(2, strips):
            @pl.when(t == feed_slot + (q_ - 2) * (chunk - HALVES))
            def _(q_=q_):
                feeds(q_)

        for q_ in detours[1:]:
            @pl.when(jnp.logical_and(helper, t == ends[q_ - 1]))
            def _(q_=q_):
                hand_over(q_)

        @pl.when(t < pieces)
        def _():
            n = pick(t, table)
            arrived(two_piece(n), two_recv.at[n])

            @pl.when(jnp.logical_and(z >= row, z < rows - 1))
            def _():
                two_up(n).start()

            @pl.when(jnp.logical_and(z <= row, z > 0))
            def _():
                two_down(n).start()

            for q_ in range(strips):
                @pl.when(t == ends[q_])
                def _(q_=q_):
                    two_swap(q_).start()

        @pl.when(t == by_kind([kind[0] for kind in kinds]))
        def _():
            finish_one()

        q, low, high = jnp.int32(0), jnp.int32(0), jnp.int32(0)
        for q_ in range(strips - 1):
            since = t - by_kind([kind[q_] for kind in kinds])
            live = jnp.logical_and(since >= 0, since < span)
            q = jnp.where(live, q_, q)
            low = jnp.where(live, since * per, low)
            high = jnp.where(live, jnp.minimum(since * per + per, parts), high)

        final = t == by_kind([kind[-1] for kind in kinds])
        q = jnp.where(final, strips - 1, q)
        low = jnp.where(final, 0, low)
        high = jnp.where(final, parts, high)

        def piece(i, _):
            correlate(q, i)
            return 0

        lax.fori_loop(low, high, piece, 0)

        @pl.when(t == open_slot)
        def _():
            arrived(two_twin, whole.at[0])
            arrived(theirs, whole.at[2])

        def second_count(t):
            ahead = t - second_lag + 1
            count = jnp.maximum(jnp.minimum(ahead, 2 * chunk), ahead - shift)
            count = jnp.maximum(count, jnp.where(soon, jnp.minimum(ahead + 1, chunk), 0))
            burst = 2 * (t - ends[-1] + 1)
            for end in ends[:-1]:
                burst = jnp.maximum(burst, 0) + jnp.where(t >= end, chunk, 0)
            count = jnp.where(last, burst, count)
            return jnp.where(t < second_slot, 0, jnp.clip(count, 0, pieces))

        def second(g, _):
            second_piece(g)
            return 0

        lax.fori_loop(second_count(t - 1), second_count(t), second, 0)

        turn = t - open_slot
        first = jnp.where(turn > 0, turn + 1, 0)
        final = jnp.where(jnp.logical_and(turn >= 0, turn < opening - 1), turn + 2, first)

        def opener(u, _):
            first_opening(u)
            return 0

        lax.fori_loop(first, final, opener, 0)

        def closer(u, _):
            first_closing(u)
            return 0

        turn = t - close_slot
        first = opening + turn
        final = jnp.where(jnp.logical_and(turn >= 0, turn < closing), first + 1, first)
        lax.fori_loop(first, final, closer, 0)
        turn = t - open_slot - opening

        @pl.when(jnp.logical_and(turn >= 0, turn < HALVES * tiles))
        def _():
            h, columns = lax.div(turn, tiles), at(lax.rem(turn, tiles) * tile, tile)
            first_own[half(h), columns] = first_tile(row, h, columns)

        for q_ in range(strips):
            @pl.when(jnp.logical_and(middle, t == home_lag + q_ * chunk + HALVES + shift + 3))
            def _(q_=q_):
                for over, _ in across:
                    arrived(passing.at[q_, over - 1], pass_recv.at[q_, over - 1])
                    pass_on(q_, over).start()

        @pl.when(t == last_slot)
        def _():
            first_last()

        return 0

    lax.fori_loop(0, slots, slot, 0)

    arrived(second_out, whole.at[4])
    arrived(first_out, load_sem.at[3])

    @pl.when(z != row)
    def _():
        arrived(two_held, sent.at[2])
        arrived(second_sent, sent.at[8])

    @pl.when(home)
    def _():
        arrived(second_sent.at[pl.ds(0, pieces - strips * HALVES)], sent.at[9])

    @pl.when(middle)
    def _():
        arrived(passing, sent.at[11])

    @pl.when(helper)
    def _():
        arrived(handed, sent.at[12])

    @pl.when(jnp.logical_and(z >= row, z < rows - 1))
    def _():
        arrived(two_own, sent.at[0])

    @pl.when(jnp.logical_and(z <= row, z > 0))
    def _():
        arrived(two_own, sent.at[1])

    arrived(two_own, sent.at[3])
    arrived(one.at[core], sent.at[4])
    arrived(weighted.at[other], sent.at[5])
    arrived(pair.at[core], sent.at[6])
    arrived(one.at[core, pl.ds(0, len(across + along))], sent.at[7])
    for block, h, target, i in relays():
        relay(block, h, target, i).wait_send()

    arrived(first_sent.at[pl.ds(0, rows - 1)], sent.at[10])


def settle_kernel(first_ref, second_ref, first_out, second_out, first, second, load, store):
    pairs = ((first_ref, first, first_out), (second_ref, second, second_out))
    part = first_ref.shape[0] // QUARTERS

    def copy(which, i, out):
        source, held, target = pairs[which]
        here = pl.ds(i * part, part)
        if out:
            return pltpu.make_async_copy(held.at[here], target.at[here], store.at[which, i])
        return pltpu.make_async_copy(source.at[here], held.at[here], load.at[which, i])

    order = [(which, i) for i in range(QUARTERS) for which in range(2)]
    for which, i in order:
        copy(which, i, False).start()
    for which, i in order:
        copy(which, i, False).wait()
        copy(which, i, True).start()
    for which, i in order:
        copy(which, i, True).wait()


def settle(first, second):
    any_space = pl.BlockSpec(memory_space=pl.ANY)
    dma = pltpu.SemaphoreType.DMA
    return pl.pallas_call(
        settle_kernel,
        out_shape=[jax.ShapeDtypeStruct(x.shape, x.dtype) for x in (first, second)],
        in_specs=[any_space] * 2,
        out_specs=[any_space] * 2,
        scratch_shapes=[pltpu.VMEM(x.shape, x.dtype) for x in (first, second)] + [dma((2, QUARTERS))] * 2,
        name="settle_grads",
    )(first, second)


def per_device(view_one, view_two, pair_weights):
    rows = lax.axis_size("row")
    samples, width = view_one.shape
    strip = min(width, 256)
    strips = width // strip
    wide, deep = PAIR, rows // PAIR
    part = samples // HALVES
    pieces = strips * rows * HALVES
    own = jax.ShapeDtypeStruct((samples, width), jnp.bfloat16)
    any_space = pl.BlockSpec(memory_space=pl.ANY)
    dma = pltpu.SemaphoreType.DMA

    def held(*shape):
        return pltpu.VMEM(shape, jnp.bfloat16)

    crossing = (wide - 1) * deep
    descent = (deep - 1) * wide
    first, second = pl.pallas_call(
        lambda *refs: step_kernel(rows, strip, *refs),
        out_shape=(own, own),
        in_specs=[any_space] * 3,
        out_specs=(any_space, any_space),
        scratch_shapes=[
            held(samples, width),
            held(rows, samples, width),
            held(rows, samples, width),
            held(strip, rows * samples),
            held(CORES, rows, samples, width),
            held(CORES, width, width),
            held(CORES, width, width),
            held(width, width),
            held(pieces, part, strip),
            held(pieces, part, strip),
            held(pieces, part, strip),
            pltpu.VMEM((part, strip), jnp.float32),
            held(rows, samples, width),
            held(crossing, part, width),
            held(descent, part, width),
            held(wide - 1, part, width),
            held(deep - 1, part, width),
            pltpu.VMEM((samples, width), jnp.float32),
            held(strips, wide - 1, part, strip),
            held((strips + 1) // 2, deep - 1, samples, strip),
            dma((4,)),
            dma((pieces,)),
            dma((rows, HALVES, max(wide, deep) - 1)),
            dma((rows, HALVES)),
            dma((pieces,)),
            dma((pieces,)),
            dma((crossing,)),
            dma((descent,)),
            dma((wide - 1,)),
            dma((deep - 1,)),
            dma((strips, wide - 1)),
            dma(((strips + 1) // 2, deep - 1, HALVES)),
            dma((13,)),
            dma((5,)),
        ],
        compiler_params=pltpu.CompilerParams(collective_id=0, has_side_effects=True, vmem_limit_bytes=62 * 2**20),
        name="twins_step",
    )(view_one, view_two, pair_weights)
    return settle(first, second)


def solution(mesh):
    placed = (P("row", "col"), P("row", "col"), P("row", "col"))
    return jax.shard_map(
        per_device,
        mesh=mesh,
        in_specs=placed,
        out_specs=(P("row", "col"), P("row", "col")),
        check_vma=False,
    )
```

```python
import jax
import jax.numpy as jnp
from jax import lax
from jax.experimental import pallas as pl
from jax.experimental.pallas import tpu as pltpu
from jax.sharding import PartitionSpec as P

MESH = pl.DeviceIdType.MESH
CORES = 2
HALVES = 2
QUARTERS = 4
PAIR = 2


def arrived(ref, sem):
    pltpu.make_async_copy(ref, ref, sem).wait()


def remote(src, dst, send, recv, device):
    return pltpu.make_async_remote_copy(
        src_ref=src, dst_ref=dst, send_sem=send, recv_sem=recv, device_id=device, device_id_type=MESH
    )


def at(start, size):
    return pl.ds(pl.multiple_of(start, size), size)


def pick(index, values):
    chosen = jnp.int32(values[0])
    for i, value in enumerate(values[1:], 1):
        chosen = jnp.where(index == i, value, chosen)
    return chosen


def step_kernel(rows, strip, one_ref, two_ref, pair_ref, first_out, second_out, two_held, two_own, two_twin, turned, one,
                pair, weighted, theirs, below, above, second_sent, second_sum, first_sent, first_wide, first_deep,
                wide_sum, deep_sum, first_own, passing, handed, load_sem, two_recv, one_send, one_recv, below_recv, above_recv, wide_recv,
                deep_recv, wide_last, deep_last, pass_recv, handed_recv, sent, whole):
    samples, width = two_ref.shape
    wide = PAIR
    deep = rows // wide
    strips = width // strip
    part = samples // HALVES
    chunk = rows * HALVES
    pieces = strips * chunk
    tile = min(width, 512)
    tiles = width // tile
    parts = CORES * tiles
    row, col = lax.axis_index("row"), lax.axis_index("col")
    z, core = lax.div(col, CORES), lax.rem(col, CORES)
    other = 1 - core
    a, b = lax.rem(row, wide), lax.div(row, wide)
    home = z == row
    reach = jnp.where(z > row, rows - 1 - row, jnp.where(z < row, row, jnp.maximum(row, rows - 1 - row)))
    back = reach - jnp.abs(z - row)
    last = back == 0
    back = rows - 1 - jnp.abs(z - row)
    twin = (row, col + 1 - 2 * core)

    def device(target, level):
        return (target, level * CORES + core)

    def half(h):
        return at(h * part, part)

    def cols(q):
        return at(q * strip, strip)

    def split(t):
        return lax.div(t, chunk), lax.rem(lax.div(t, HALVES), rows), lax.rem(t, HALVES)

    across = [(over, 0) for over in range(1, wide)]
    along = [(0, down) for down in range(1, deep)]
    far = [(over, down) for over in range(1, wide) for down in range(1, deep)]
    sources = [(0, 0)] + across + along + far
    targets = far + across + along + [(0, 0)]

    def block_of(over, down):
        return lax.rem(b + down, deep) * wide + lax.rem(a + over, wide)

    def choose(i, pairs):
        return block_of(pick(i, [over for over, _ in pairs]), pick(i, [down for _, down in pairs]))

    def two_piece(t):
        q, i, h = split(t)
        return two_own.at[choose(i, sources), half(h), cols(q)]

    def two_up(t):
        return remote(two_piece(t), two_piece(t), sent.at[0], two_recv.at[t], device(row, z + 1))

    def two_down(t):
        return remote(two_piece(t), two_piece(t), sent.at[1], two_recv.at[t], device(row, z - 1))

    def feed(q, h):
        over = lax.rem(a - lax.rem(z, wide) + wide, wide)
        down = lax.rem(b - lax.div(z, wide) + deep, deep)
        place = pick(over * deep + down, [sources.index((o, d)) for o in range(wide) for d in range(deep)])
        t = q * chunk + place * HALVES + h
        return remote(two_held.at[half(h), cols(q)], two_own.at[row, half(h), cols(q)], sent.at[2],
                      two_recv.at[t], device(z, z))

    def own_two(q, h):
        return pltpu.make_async_copy(two_ref.at[half(h), cols(q)], two_own.at[row, half(h), cols(q)],
                                     two_recv.at[q * chunk + h])

    home_a, home_b = lax.rem(z, wide), lax.div(z, wide)
    remote_a, remote_b = a != home_a, b != home_b

    home_a, home_b = lax.rem(z, wide), lax.div(z, wide)
    remote_a, remote_b = a != home_a, b != home_b
    opposite = jnp.logical_and(remote_a, remote_b)
    helper = jnp.logical_and(remote_a, jnp.logical_not(remote_b))
    detours = list(range(0, strips, 2))

    def hand(q, h):
        place = lax.rem(b - home_b + deep, deep) - 1
        n = detours.index(q)
        return remote(two_held.at[half(h), cols(q)], handed.at[n, place, half(h)], sent.at[2],
                      handed_recv.at[n, place, h], device(home_b * wide + a, z))

    def hand_on(q, down, h):
        over = lax.rem(a - home_a + wide, wide)
        place = pick(over, [sources.index((max(o, 1), down)) for o in range(wide)])
        n = detours.index(q)
        return remote(handed.at[n, down - 1, half(h)], two_own.at[block_of(0, down), half(h), cols(q)], sent.at[12],
                      two_recv.at[q * chunk + place * HALVES + h], device(z, z))

    def hand_over(q):
        for _, down in along:
            for h in range(HALVES):
                arrived(handed.at[detours.index(q), down - 1, half(h)], handed_recv.at[detours.index(q), down - 1, h])
                hand_on(q, down, h).start()

    def feeds(q):
        direct = jnp.logical_and(z != row, jnp.logical_not(opposite)) if q in detours else z != row

        @pl.when(direct)
        def _():
            for h in range(HALVES):
                feed(q, h).start()

        if q in detours:
            @pl.when(opposite)
            def _():
                for h in range(HALVES):
                    hand(q, h).start()

    def two_swap(q):
        return remote(two_own.at[:, :, cols(q)], two_twin.at[:, :, cols(q)], sent.at[3], whole.at[0], twin)

    def one_block(block, h):
        return one.at[core, block, half(h)]

    def one_copy(block, h, target, send):
        return remote(one_block(block, h), one_block(block, h), send, one_recv.at[block, h], (target, col))

    def one_swap(block, h):
        return remote(one_block(block, h), one_block(block, h), sent.at[4], whole.at[1], twin)

    def take_one(block, h):
        arrived(one_block(block, h), one_recv.at[block, h])
        one_swap(block, h).start()

    def weights_swap():
        return remote(pair_ref.at[at(other * width, width)], pair.at[core], sent.at[6], whole.at[3], twin)

    def theirs_swap(q):
        return remote(weighted.at[other, cols(q)], theirs.at[cols(q)], sent.at[5], whole.at[2], twin)

    load_two = pltpu.make_async_copy(two_ref, two_held, load_sem.at[0])
    load_one = pltpu.make_async_copy(one_ref, one.at[core, row], load_sem.at[1])
    load_pair = pltpu.make_async_copy(pair_ref.at[at(core * width, width)], pair.at[core], load_sem.at[2])

    load_two.start()

    @pl.when(home)
    def _():
        for q in range(strips):
            for h in range(HALVES):
                own_two(q, h).start()

    load_one.start()
    load_pair.start()

    barrier = pltpu.get_barrier_semaphore()

    def greet(target):
        pl.semaphore_signal(barrier, inc=1, device_id=target, device_id_type=MESH)

    greet(twin)
    for step in range(1, rows):
        greet((lax.rem(row + step, rows), col))

    @pl.when(z > 0)
    def _():
        greet(device(row, z - 1))

    @pl.when(z < rows - 1)
    def _():
        greet(device(row, z + 1))

    pl.semaphore_wait(barrier, rows + jnp.where(z > 0, 1, 0) + jnp.where(z < rows - 1, 1, 0))
    load_two.wait()

    feeds(0)
    load_one.wait()
    early = [(0, block_of(over, down)) for over, down in across] + [(1, block_of(over, down)) for over, down in along]
    late = [(1, block_of(over, down)) for over, down in across] + [(0, block_of(over, down)) for over, down in along]
    for h, target in early + late:
        @pl.when(target != z)
        def _(h=h, target=target):
            one_copy(row, h, target, sent.at[7]).start()
    for h in range(HALVES):
        one_swap(row, h).start()
    weights_swap().start()

    @pl.when(helper)
    def _():
        hand_over(0)

    for h, target in early:
        @pl.when(target == z)
        def _(h=h, target=target):
            one_copy(row, h, target, sent.at[7]).start()

    def relays():
        found = []
        for over, down in across:
            for i, (_, other_down) in enumerate(along):
                target = block_of(0, other_down)
                found.append((block_of(over, down), 0, target, i))
        for over, down in along:
            for i, (other_over, _) in enumerate(across):
                target = block_of(other_over, 0)
                found.append((block_of(over, down), 1, target, i))
        return found

    def relay(block, h, target, i):
        return one_copy(block, h, target, one_send.at[block, h, i])

    def relay_one():
        if strips > 1:
            feeds(1)
        for over, down in across:
            take_one(block_of(over, down), 0)
        for over, down in along:
            take_one(block_of(over, down), 1)
        for block, h, target, i in relays():
            @pl.when(target != z)
            def _(block=block, h=h, target=target, i=i):
                relay(block, h, target, i).start()
        for h, target in late:
            @pl.when(target == z)
            def _(h=h, target=target):
                one_copy(row, h, target, sent.at[7]).start()
        for block, h, target, i in relays():
            @pl.when(target == z)
            def _(block=block, h=h, target=target, i=i):
                relay(block, h, target, i).start()

    def take_more():
        for over, down in across:
            take_one(block_of(over, down), 1)
        for over, down in along:
            take_one(block_of(over, down), 0)

    def finish_one():
        for over, down in far:
            take_one(block_of(over, down), 0)
            take_one(block_of(over, down), 1)
        arrived(one.at[other], whole.at[1])
        load_pair.wait()
        arrived(pair.at[other], whole.at[3])

    def correlate(q, p):
        side, i = lax.div(p, tiles), lax.rem(p, tiles)

        @pl.when(p == 0)
        def _():
            turned[...] = two_own[:, :, cols(q)].reshape(rows * samples, strip).T

        columns = at(i * tile, tile)
        total = jnp.dot(turned[...], one[side, :, :, columns].reshape(rows * samples, tile),
                        preferred_element_type=jnp.float32)
        row_ids = (row * CORES + core) * width + q * strip + lax.broadcasted_iota(jnp.int32, total.shape, 0)
        col_ids = (z * CORES + side) * width + i * tile + lax.broadcasted_iota(jnp.int32, total.shape, 1)
        identity = jnp.where(row_ids == col_ids, 1.0, 0.0).astype(jnp.float32)
        scale = pair[side, cols(q), columns].astype(jnp.float32)
        weighted[side, cols(q), columns] = (scale * (total / (rows * samples) - identity)).astype(jnp.bfloat16)

        @pl.when(p == parts - 1)
        def _():
            theirs_swap(q).start()

    def chain_up(g):
        return remote(second_sent.at[g], below.at[g], sent.at[8], below_recv.at[g], device(row, z + 1))

    def chain_down(g):
        return remote(second_sent.at[g], above.at[g], sent.at[8], above_recv.at[g], device(row, z - 1))

    def spread(g):
        q, i, h = split(g)
        return remote(second_sent.at[g], second_out.at[half(h), cols(q)], sent.at[9], whole.at[4],
                      device(choose(i, targets), z))

    def via(g):
        q, i, h = split(g)
        return remote(second_sent.at[g], passing.at[q, pick(i, [over for over, _ in targets]) - 1], sent.at[9],
                      pass_recv.at[q, pick(i, [over for over, _ in targets]) - 1],
                      device(block_of(0, pick(i, [down for _, down in targets])), z))

    def pass_on(q, over):
        return remote(passing.at[q, over - 1], second_out.at[half(HALVES - 1), cols(q)], sent.at[11], whole.at[4],
                      device(block_of(over, 0), z))

    middle = jnp.logical_and(a == lax.rem(z, wide), b != lax.div(z, wide))

    from_below = jnp.logical_and(z > 0, z <= row)
    from_above = jnp.logical_and(z < rows - 1, z >= row)

    def second_piece(g):
        q, i, h = split(g)
        target = choose(i, targets)
        contract = (((1,), (1,)), ((), ()))
        second_sum[...] = (
            lax.dot_general(one[0, target, half(h)], weighted[0, cols(q)], contract, preferred_element_type=jnp.float32)
            + lax.dot_general(one[1, target, half(h)], weighted[1, cols(q)], contract,
                              preferred_element_type=jnp.float32))

        @pl.when(from_below)
        def _():
            arrived(below.at[g], below_recv.at[g])
            second_sum[...] += below[g].astype(jnp.float32)

        @pl.when(from_above)
        def _():
            arrived(above.at[g], above_recv.at[g])
            second_sum[...] += above[g].astype(jnp.float32)

        keep = jnp.logical_and(home, i == rows - 1)

        second_sent[g] = second_sum[...].astype(jnp.bfloat16)

        @pl.when(keep)
        def _():
            pltpu.make_async_copy(second_sent.at[g], second_out.at[half(h), cols(q)], whole.at[4]).start()

        @pl.when(z < row)
        def _():
            chain_up(g).start()

        @pl.when(z > row)
        def _():
            chain_down(g).start()

        turned_off = jnp.logical_and(h == HALVES - 1, i < len(far))

        @pl.when(jnp.logical_and(home, turned_off))
        def _():
            via(g).start()

        @pl.when(jnp.logical_and(home, jnp.logical_not(jnp.logical_or(turned_off, i == rows - 1))))
        def _():
            spread(g).start()

    lead = [(0, over, down) for over, _ in across for down in range(deep)]
    lead_deep = [(1, over, down) for _, down in along for over in range(wide)]
    order = []
    for i in range(max(len(lead), len(lead_deep))):
        order += lead[::-1][i:i + 1] + lead_deep[::-1][i:i + 1]
    opening = len(order)
    order += [(0, 0, down) for _, down in along] + [(1, over, 0) for over, _ in across] + [(0, 0, 0), (1, 0, 0)]

    def unit(u):
        h = pick(u, [entry[0] for entry in order])
        over = pick(u, [entry[1] for entry in order])
        down = pick(u, [entry[2] for entry in order])
        return h, over, down, block_of(over, down)

    def first_hop(u):
        h, over, down, target = unit(u)
        flat = jnp.where(h == 0, (over - 1) * deep + lax.div(target, wide), (down - 1) * wide + lax.rem(target, wide))
        return h, over, down, target, flat

    def wide_open(u):
        h, over, down, target, flat = first_hop(u)
        return remote(first_sent.at[target, half(h)], first_wide.at[flat], sent.at[10], wide_recv.at[flat],
                      (b * wide + lax.rem(a + over, wide), col))

    def deep_open(u):
        h, over, down, target, flat = first_hop(u)
        return remote(first_sent.at[target, half(h)], first_deep.at[flat], sent.at[10], deep_recv.at[flat],
                      (lax.rem(b + down, deep) * wide + a, col))

    def deep_close(u):
        h, over, down, target = unit(u)
        return remote(first_sent.at[target, half(h)], deep_sum.at[down - 1], sent.at[10], deep_last.at[down - 1],
                      (target, col))

    def wide_close(u):
        h, over, down, target = unit(u)
        return remote(first_sent.at[target, half(h)], wide_sum.at[over - 1], sent.at[10], wide_last.at[over - 1],
                      (target, col))

    def first_tile(target, h, columns):
        return (jnp.dot(two_own[target, half(h)], weighted[core, :, columns], preferred_element_type=jnp.float32)
                + jnp.dot(two_twin[target, half(h)], theirs[:, columns], preferred_element_type=jnp.float32))

    def first_opening(u):
        h, over, down, target = unit(u)

        def body(i, _):
            columns = at(i * tile, tile)
            first_sent[target, half(h), columns] = first_tile(target, h, columns).astype(jnp.bfloat16)
            return 0

        lax.fori_loop(0, tiles, body, 0)

        @pl.when(h == 0)
        def _():
            wide_open(u).start()

        @pl.when(h == 1)
        def _():
            deep_open(u).start()

    def first_closing(u):
        h, over, down, target = unit(u)

        @pl.when(h == 0)
        def _():
            for over_ in range(1, wide):
                flat = (over_ - 1) * deep + lax.div(target, wide)
                arrived(first_wide.at[flat], wide_recv.at[flat])

        @pl.when(h == 1)
        def _():
            for down_ in range(1, deep):
                flat = (down_ - 1) * wide + lax.rem(target, wide)
                arrived(first_deep.at[flat], deep_recv.at[flat])

        def body(i, _):
            columns = at(i * tile, tile)
            total = first_tile(target, h, columns)

            @pl.when(h == 0)
            def _():
                acc = total
                for over_ in range(1, wide):
                    acc += first_wide[(over_ - 1) * deep + lax.div(target, wide), :, columns].astype(jnp.float32)
                first_sent[target, half(h), columns] = acc.astype(jnp.bfloat16)

            @pl.when(h == 1)
            def _():
                acc = total
                for down_ in range(1, deep):
                    acc += first_deep[(down_ - 1) * wide + lax.rem(target, wide), :, columns].astype(jnp.float32)
                first_sent[target, half(h), columns] = acc.astype(jnp.bfloat16)

            return 0

        lax.fori_loop(0, tiles, body, 0)

        @pl.when(h == 0)
        def _():
            deep_close(u).start()

        @pl.when(h == 1)
        def _():
            wide_close(u).start()

    def first_last():
        for _, down in along:
            arrived(deep_sum.at[down - 1], deep_last.at[down - 1])
        for over, _ in across:
            arrived(wide_sum.at[over - 1], wide_last.at[over - 1])
            for d in range(deep):
                @pl.when(d == b)
                def _(over=over, d=d):
                    flat = (over - 1) * deep + d
                    arrived(first_wide.at[flat], wide_recv.at[flat])
        for _, down in along:
            for o in range(wide):
                @pl.when(o == a)
                def _(down=down, o=o):
                    flat = (down - 1) * wide + o
                    arrived(first_deep.at[flat], deep_recv.at[flat])

        def finish_first(i, _):
            columns = at(i * tile, tile)
            top = first_own[half(0), columns]
            for over, _ in across:
                top += first_wide[(over - 1) * deep + b, :, columns].astype(jnp.float32)
            for _, down in along:
                top += deep_sum[down - 1, :, columns].astype(jnp.float32)
            first_sent[row, half(0), columns] = top.astype(jnp.bfloat16)
            low = first_own[half(1), columns]
            for _, down in along:
                low += first_deep[(down - 1) * wide + a, :, columns].astype(jnp.float32)
            for over, _ in across:
                low += wide_sum[over - 1, :, columns].astype(jnp.float32)
            first_sent[row, half(1), columns] = low.astype(jnp.bfloat16)
            return 0

        lax.fori_loop(0, tiles, finish_first, 0)
        pltpu.make_async_copy(first_sent.at[row], first_out, load_sem.at[3]).start()

    closing = len(order) - 2 - opening
    def run(q, order):
        return [q * chunk + sources.index(pair) * HALVES + h for pair in order for h in range(HALVES)]

    table = run(0, sources)
    ends = [chunk - 1]
    for q in range(1, strips):
        if q <= 2:
            for owned in [1] if q == 1 else range(2, strips):
                table += run(owned, [(0, 0)])
        table += run(q, sources[1:])
        ends.append(len(table) - 1)
    shift = max(end - (q + 1) * chunk + 1 for q, end in enumerate(ends))
    soon = jnp.logical_and(back == 1, jnp.logical_not(last))
    def starts(first_lag, later_lag, length):
        found = []
        for q, end in enumerate(ends):
            begin = end + (later_lag if q else first_lag)
            if q + 1 == strips:
                begin = end + (length > 1)
            found.append(max(begin, found[-1] + length) if found else begin)
        return found

    kinds = [starts(0, 0, 1), starts(4, 0, (parts + 1) // 2), starts(6, 2, (parts + 1) // 2), [ends[0] + 14]]
    kinds[3] += [max(ends[min(2, strips - 1)], kinds[3][0]) + q for q in range(1, strips - 1)]
    kinds[3].append(max(ends[-1], kinds[3][-1] + 1))

    def by_kind(values):
        return jnp.where(last, values[0], jnp.where(soon, values[1], jnp.where(home, values[3], values[2])))

    per = by_kind([parts, 2, 2, parts])
    span = by_kind([1, (parts + 1) // 2, (parts + 1) // 2, 1])
    home_lag = max(kinds[3][0] + 2, chunk + 4 * (rows - 1))
    second_lag = jnp.where(last, chunk - 1, jnp.where(home, home_lag, chunk + 4 * back))
    second_slot = by_kind([kind[0] for kind in kinds]) + jnp.where(jnp.logical_or(last, home), 0, span)
    open_slot = by_kind([kind[-1] for kind in kinds]) + 2
    open_limit = max(kind[-1] for kind in kinds) + 1 + opening
    close_slot = open_limit + by_kind([6, 4, 6, 11])
    relay_slot = pick(jnp.abs(z - row), [8, 4, 2] + [1] * rows)
    feed_slot = chunk + 1 - jnp.minimum(jnp.abs(z - row), 4)
    slots = pieces + 1 + home_lag + shift
    last_slot = slots - 1
    each = (opening + 1) // 2

    def slot(t, _):
        @pl.when(t == relay_slot)
        def _():
            relay_one()

        for q_ in range(2, strips):
            @pl.when(t == feed_slot + (q_ - 2) * (chunk - HALVES))
            def _(q_=q_):
                feeds(q_)

        for q_ in detours[1:]:
            @pl.when(jnp.logical_and(helper, t == ends[q_ - 1]))
            def _(q_=q_):
                hand_over(q_)

        @pl.when(t < pieces)
        def _():
            n = pick(t, table)
            arrived(two_piece(n), two_recv.at[n])

            @pl.when(jnp.logical_and(z >= row, z < rows - 1))
            def _():
                two_up(n).start()

            @pl.when(jnp.logical_and(z <= row, z > 0))
            def _():
                two_down(n).start()

            for q_ in range(strips):
                @pl.when(t == ends[q_])
                def _(q_=q_):
                    two_swap(q_).start()

        @pl.when(t == by_kind([chunk - 2, chunk + 1, chunk + 2, kinds[3][0] - 2]))
        def _():
            take_more()

        @pl.when(t == by_kind([kind[0] for kind in kinds]))
        def _():
            finish_one()

        q, low, high = jnp.int32(0), jnp.int32(0), jnp.int32(0)
        for q_ in range(strips - 1):
            since = t - by_kind([kind[q_] for kind in kinds])
            live = jnp.logical_and(since >= 0, since < span)
            q = jnp.where(live, q_, q)
            low = jnp.where(live, since * per, low)
            high = jnp.where(live, jnp.minimum(since * per + per, parts), high)

        final = t == by_kind([kind[-1] for kind in kinds])
        q = jnp.where(final, strips - 1, q)
        low = jnp.where(final, 0, low)
        high = jnp.where(final, parts, high)

        def piece(i, _):
            correlate(q, i)
            return 0

        lax.fori_loop(low, high, piece, 0)

        @pl.when(t == open_slot)
        def _():
            arrived(two_twin, whole.at[0])
            arrived(theirs, whole.at[2])

        def second_count(t):
            ahead = t - second_lag + 1
            count = jnp.maximum(jnp.minimum(ahead, 2 * chunk), ahead - shift)
            count = jnp.maximum(count, jnp.where(soon, jnp.minimum(ahead + 1, chunk), 0))
            burst = 2 * (t - ends[-1] + 1)
            for end in ends[:-1]:
                burst = jnp.maximum(burst, 0) + jnp.where(t >= end, chunk, 0)
            count = jnp.where(last, burst, count)
            return jnp.where(t < second_slot, 0, jnp.clip(count, 0, pieces))

        def second(g, _):
            second_piece(g)
            return 0

        lax.fori_loop(second_count(t - 1), second_count(t), second, 0)

        turn = t - open_slot
        first = jnp.where(turn > 0, turn + 1, 0)
        final = jnp.where(jnp.logical_and(turn >= 0, turn < opening - 1), turn + 2, first)

        def opener(u, _):
            first_opening(u)
            return 0

        lax.fori_loop(first, final, opener, 0)

        def closer(u, _):
            first_closing(u)
            return 0

        turn = t - close_slot
        first = opening + turn
        final = jnp.where(jnp.logical_and(turn >= 0, turn < closing), first + 1, first)
        lax.fori_loop(first, final, closer, 0)
        turn = t - open_slot - opening

        @pl.when(jnp.logical_and(turn >= 0, turn < HALVES * tiles))
        def _():
            h, columns = lax.div(turn, tiles), at(lax.rem(turn, tiles) * tile, tile)
            first_own[half(h), columns] = first_tile(row, h, columns)

        for q_ in range(strips):
            @pl.when(jnp.logical_and(middle, t == home_lag + q_ * chunk + HALVES + shift + 3))
            def _(q_=q_):
                for over, _ in across:
                    arrived(passing.at[q_, over - 1], pass_recv.at[q_, over - 1])
                    pass_on(q_, over).start()

        @pl.when(t == last_slot)
        def _():
            first_last()

        return 0

    lax.fori_loop(0, slots, slot, 0)

    arrived(second_out, whole.at[4])
    arrived(first_out, load_sem.at[3])

    @pl.when(z != row)
    def _():
        arrived(two_held, sent.at[2])
        arrived(second_sent, sent.at[8])

    @pl.when(home)
    def _():
        arrived(second_sent.at[pl.ds(0, pieces - strips * HALVES)], sent.at[9])

    @pl.when(middle)
    def _():
        arrived(passing, sent.at[11])

    @pl.when(helper)
    def _():
        arrived(handed, sent.at[12])

    @pl.when(jnp.logical_and(z >= row, z < rows - 1))
    def _():
        arrived(two_own, sent.at[0])

    @pl.when(jnp.logical_and(z <= row, z > 0))
    def _():
        arrived(two_own, sent.at[1])

    arrived(two_own, sent.at[3])
    arrived(one.at[core], sent.at[4])
    arrived(weighted.at[other], sent.at[5])
    arrived(pair.at[core], sent.at[6])
    arrived(one.at[core, pl.ds(0, len(across + along))], sent.at[7])
    for block, h, target, i in relays():
        relay(block, h, target, i).wait_send()

    arrived(first_sent.at[pl.ds(0, rows - 1)], sent.at[10])


def settle_kernel(first_ref, second_ref, first_out, second_out, first, second, load, store):
    pairs = ((first_ref, first, first_out), (second_ref, second, second_out))
    part = first_ref.shape[0] // QUARTERS

    def copy(which, i, out):
        source, held, target = pairs[which]
        here = pl.ds(i * part, part)
        if out:
            return pltpu.make_async_copy(held.at[here], target.at[here], store.at[which, i])
        return pltpu.make_async_copy(source.at[here], held.at[here], load.at[which, i])

    order = [(which, i) for i in range(QUARTERS) for which in range(2)]
    for which, i in order:
        copy(which, i, False).start()
    for which, i in order:
        copy(which, i, False).wait()
        copy(which, i, True).start()
    for which, i in order:
        copy(which, i, True).wait()


def settle(first, second):
    any_space = pl.BlockSpec(memory_space=pl.ANY)
    dma = pltpu.SemaphoreType.DMA
    return pl.pallas_call(
        settle_kernel,
        out_shape=[jax.ShapeDtypeStruct(x.shape, x.dtype) for x in (first, second)],
        in_specs=[any_space] * 2,
        out_specs=[any_space] * 2,
        scratch_shapes=[pltpu.VMEM(x.shape, x.dtype) for x in (first, second)] + [dma((2, QUARTERS))] * 2,
        name="settle_grads",
    )(first, second)


def per_device(view_one, view_two, pair_weights):
    rows = lax.axis_size("row")
    samples, width = view_one.shape
    strip = min(width, 256)
    strips = width // strip
    wide, deep = PAIR, rows // PAIR
    part = samples // HALVES
    pieces = strips * rows * HALVES
    own = jax.ShapeDtypeStruct((samples, width), jnp.bfloat16)
    any_space = pl.BlockSpec(memory_space=pl.ANY)
    dma = pltpu.SemaphoreType.DMA

    def held(*shape):
        return pltpu.VMEM(shape, jnp.bfloat16)

    crossing = (wide - 1) * deep
    descent = (deep - 1) * wide
    first, second = pl.pallas_call(
        lambda *refs: step_kernel(rows, strip, *refs),
        out_shape=(own, own),
        in_specs=[any_space] * 3,
        out_specs=(any_space, any_space),
        scratch_shapes=[
            held(samples, width),
            held(rows, samples, width),
            held(rows, samples, width),
            held(strip, rows * samples),
            held(CORES, rows, samples, width),
            held(CORES, width, width),
            held(CORES, width, width),
            held(width, width),
            held(pieces, part, strip),
            held(pieces, part, strip),
            held(pieces, part, strip),
            pltpu.VMEM((part, strip), jnp.float32),
            held(rows, samples, width),
            held(crossing, part, width),
            held(descent, part, width),
            held(wide - 1, part, width),
            held(deep - 1, part, width),
            pltpu.VMEM((samples, width), jnp.float32),
            held(strips, wide - 1, part, strip),
            held((strips + 1) // 2, deep - 1, samples, strip),
            dma((4,)),
            dma((pieces,)),
            dma((rows, HALVES, max(wide, deep) - 1)),
            dma((rows, HALVES)),
            dma((pieces,)),
            dma((pieces,)),
            dma((crossing,)),
            dma((descent,)),
            dma((wide - 1,)),
            dma((deep - 1,)),
            dma((strips, wide - 1)),
            dma(((strips + 1) // 2, deep - 1, HALVES)),
            dma((13,)),
            dma((5,)),
        ],
        compiler_params=pltpu.CompilerParams(collective_id=0, has_side_effects=True, vmem_limit_bytes=62 * 2**20),
        name="twins_step",
    )(view_one, view_two, pair_weights)
    return settle(first, second)


def solution(mesh):
    placed = (P("row", "col"), P("row", "col"), P("row", "col"))
    return jax.shard_map(
        per_device,
        mesh=mesh,
        in_specs=placed,
        out_specs=(P("row", "col"), P("row", "col")),
        check_vma=False,
    )
```

```python
import jax
import jax.numpy as jnp
from jax import lax
from jax.experimental import pallas as pl
from jax.experimental.pallas import tpu as pltpu
from jax.sharding import PartitionSpec as P

MESH = pl.DeviceIdType.MESH
CORES = 2
HALVES = 2
QUARTERS = 4
PAIR = 2


def arrived(ref, sem):
    pltpu.make_async_copy(ref, ref, sem).wait()


def remote(src, dst, send, recv, device):
    return pltpu.make_async_remote_copy(
        src_ref=src, dst_ref=dst, send_sem=send, recv_sem=recv, device_id=device, device_id_type=MESH
    )


def at(start, size):
    return pl.ds(pl.multiple_of(start, size), size)


def pick(index, values):
    chosen = jnp.int32(values[0])
    for i, value in enumerate(values[1:], 1):
        chosen = jnp.where(index == i, value, chosen)
    return chosen


def step_kernel(rows, strip, one_ref, two_ref, pair_ref, first_out, second_out, two_held, two_own, two_twin, turned, one,
                pair, weighted, theirs, below, above, second_sent, second_sum, first_sent, first_wide, first_deep,
                wide_sum, deep_sum, first_own, passing, handed, load_sem, two_recv, one_send, one_recv, below_recv, above_recv, wide_recv,
                deep_recv, wide_last, deep_last, pass_recv, handed_recv, sent, whole):
    samples, width = two_ref.shape
    wide = PAIR
    deep = rows // wide
    strips = width // strip
    part = samples // HALVES
    chunk = rows * HALVES
    pieces = strips * chunk
    tile = min(width, 512)
    tiles = width // tile
    parts = CORES * tiles
    row, col = lax.axis_index("row"), lax.axis_index("col")
    z, core = lax.div(col, CORES), lax.rem(col, CORES)
    other = 1 - core
    a, b = lax.rem(row, wide), lax.div(row, wide)
    home = z == row
    reach = jnp.where(z > row, rows - 1 - row, jnp.where(z < row, row, jnp.maximum(row, rows - 1 - row)))
    back = reach - jnp.abs(z - row)
    last = back == 0
    back = rows - 1 - jnp.abs(z - row)
    twin = (row, col + 1 - 2 * core)

    def device(target, level):
        return (target, level * CORES + core)

    def half(h):
        return at(h * part, part)

    def cols(q):
        return at(q * strip, strip)

    def split(t):
        return lax.div(t, chunk), lax.rem(lax.div(t, HALVES), rows), lax.rem(t, HALVES)

    across = [(over, 0) for over in range(1, wide)]
    along = [(0, down) for down in range(1, deep)]
    far = [(over, down) for over in range(1, wide) for down in range(1, deep)]
    sources = [(0, 0)] + across + along + far
    targets = far + across + along + [(0, 0)]

    def block_of(over, down):
        return lax.rem(b + down, deep) * wide + lax.rem(a + over, wide)

    def choose(i, pairs):
        return block_of(pick(i, [over for over, _ in pairs]), pick(i, [down for _, down in pairs]))

    def two_piece(t):
        q, i, h = split(t)
        return two_own.at[choose(i, sources), half(h), cols(q)]

    def two_up(t):
        return remote(two_piece(t), two_piece(t), sent.at[0], two_recv.at[t], device(row, z + 1))

    def two_down(t):
        return remote(two_piece(t), two_piece(t), sent.at[1], two_recv.at[t], device(row, z - 1))

    def feed(q, h):
        over = lax.rem(a - lax.rem(z, wide) + wide, wide)
        down = lax.rem(b - lax.div(z, wide) + deep, deep)
        place = pick(over * deep + down, [sources.index((o, d)) for o in range(wide) for d in range(deep)])
        t = q * chunk + place * HALVES + h
        return remote(two_held.at[half(h), cols(q)], two_own.at[row, half(h), cols(q)], sent.at[2],
                      two_recv.at[t], device(z, z))

    def own_two(q, h):
        return pltpu.make_async_copy(two_ref.at[half(h), cols(q)], two_own.at[row, half(h), cols(q)],
                                     two_recv.at[q * chunk + h])

    home_a, home_b = lax.rem(z, wide), lax.div(z, wide)
    remote_a, remote_b = a != home_a, b != home_b

    home_a, home_b = lax.rem(z, wide), lax.div(z, wide)
    remote_a, remote_b = a != home_a, b != home_b
    opposite = jnp.logical_and(remote_a, remote_b)
    helper = jnp.logical_and(remote_a, jnp.logical_not(remote_b))
    detours = list(range(0, strips, 2))

    def hand(q, h):
        place = lax.rem(b - home_b + deep, deep) - 1
        n = detours.index(q)
        return remote(two_held.at[half(h), cols(q)], handed.at[n, place, half(h)], sent.at[2],
                      handed_recv.at[n, place, h], device(home_b * wide + a, z))

    def hand_on(q, down, h):
        over = lax.rem(a - home_a + wide, wide)
        place = pick(over, [sources.index((max(o, 1), down)) for o in range(wide)])
        n = detours.index(q)
        return remote(handed.at[n, down - 1, half(h)], two_own.at[block_of(0, down), half(h), cols(q)], sent.at[12],
                      two_recv.at[q * chunk + place * HALVES + h], device(z, z))

    def hand_over(q):
        for _, down in along:
            for h in range(HALVES):
                arrived(handed.at[detours.index(q), down - 1, half(h)], handed_recv.at[detours.index(q), down - 1, h])
                hand_on(q, down, h).start()

    def feeds(q):
        direct = jnp.logical_and(z != row, jnp.logical_not(opposite)) if q in detours else z != row

        @pl.when(direct)
        def _():
            for h in range(HALVES):
                feed(q, h).start()

        if q in detours:
            @pl.when(opposite)
            def _():
                for h in range(HALVES):
                    hand(q, h).start()

    def two_swap(q):
        return remote(two_own.at[:, :, cols(q)], two_twin.at[:, :, cols(q)], sent.at[3], whole.at[0], twin)

    def one_block(block, h):
        return one.at[core, block, half(h)]

    def one_copy(block, h, target, send):
        return remote(one_block(block, h), one_block(block, h), send, one_recv.at[block, h], (target, col))

    def one_swap(block, h):
        return remote(one_block(block, h), one_block(block, h), sent.at[4], whole.at[1], twin)

    def take_one(block, h):
        arrived(one_block(block, h), one_recv.at[block, h])
        one_swap(block, h).start()

    def weights_swap():
        return remote(pair_ref.at[at(other * width, width)], pair.at[core], sent.at[6], whole.at[3], twin)

    def theirs_swap(q):
        return remote(weighted.at[other, cols(q)], theirs.at[cols(q)], sent.at[5], whole.at[2], twin)

    load_two = pltpu.make_async_copy(two_ref, two_held, load_sem.at[0])
    load_one = pltpu.make_async_copy(one_ref, one.at[core, row], load_sem.at[1])
    load_pair = pltpu.make_async_copy(pair_ref.at[at(core * width, width)], pair.at[core], load_sem.at[2])

    load_two.start()

    @pl.when(home)
    def _():
        for q in range(strips):
            for h in range(HALVES):
                own_two(q, h).start()

    load_one.start()
    load_pair.start()

    barrier = pltpu.get_barrier_semaphore()

    def greet(target):
        pl.semaphore_signal(barrier, inc=1, device_id=target, device_id_type=MESH)

    greet(twin)
    for step in range(1, rows):
        greet((lax.rem(row + step, rows), col))

    @pl.when(z > 0)
    def _():
        greet(device(row, z - 1))

    @pl.when(z < rows - 1)
    def _():
        greet(device(row, z + 1))

    pl.semaphore_wait(barrier, rows + jnp.where(z > 0, 1, 0) + jnp.where(z < rows - 1, 1, 0))
    load_two.wait()

    feeds(0)
    load_one.wait()
    early = [(0, block_of(over, down)) for over, down in across] + [(1, block_of(over, down)) for over, down in along]
    late = [(1, block_of(over, down)) for over, down in across] + [(0, block_of(over, down)) for over, down in along]
    for h, target in early + late:
        @pl.when(target != z)
        def _(h=h, target=target):
            one_copy(row, h, target, sent.at[7]).start()
    for h in range(HALVES):
        one_swap(row, h).start()
    weights_swap().start()

    @pl.when(helper)
    def _():
        hand_over(0)

    for h, target in early:
        @pl.when(target == z)
        def _(h=h, target=target):
            one_copy(row, h, target, sent.at[7]).start()

    def relays():
        found = []
        for over, down in across:
            for i, (_, other_down) in enumerate(along):
                target = block_of(0, other_down)
                found.append((block_of(over, down), 0, target, i))
        for over, down in along:
            for i, (other_over, _) in enumerate(across):
                target = block_of(other_over, 0)
                found.append((block_of(over, down), 1, target, i))
        return found

    def relay(block, h, target, i):
        return one_copy(block, h, target, one_send.at[block, h, i])

    def relay_one():
        if strips > 1:
            feeds(1)
        for over, down in across:
            take_one(block_of(over, down), 0)
        for over, down in along:
            take_one(block_of(over, down), 1)
        for block, h, target, i in relays():
            @pl.when(target != z)
            def _(block=block, h=h, target=target, i=i):
                relay(block, h, target, i).start()
        for h, target in late:
            @pl.when(target == z)
            def _(h=h, target=target):
                one_copy(row, h, target, sent.at[7]).start()
        for block, h, target, i in relays():
            @pl.when(target == z)
            def _(block=block, h=h, target=target, i=i):
                relay(block, h, target, i).start()

    def take_more():
        for over, down in across:
            take_one(block_of(over, down), 1)
        for over, down in along:
            take_one(block_of(over, down), 0)

    def finish_one():
        for over, down in far:
            take_one(block_of(over, down), 0)
            take_one(block_of(over, down), 1)
        arrived(one.at[other], whole.at[1])
        load_pair.wait()
        arrived(pair.at[other], whole.at[3])

    def correlate(q, p):
        side, i = lax.div(p, tiles), lax.rem(p, tiles)

        @pl.when(p == 0)
        def _():
            turned[...] = two_own[:, :, cols(q)].reshape(rows * samples, strip).T

        columns = at(i * tile, tile)
        total = jnp.dot(turned[...], one[side, :, :, columns].reshape(rows * samples, tile),
                        preferred_element_type=jnp.float32)
        row_ids = (row * CORES + core) * width + q * strip + lax.broadcasted_iota(jnp.int32, total.shape, 0)
        col_ids = (z * CORES + side) * width + i * tile + lax.broadcasted_iota(jnp.int32, total.shape, 1)
        identity = jnp.where(row_ids == col_ids, 1.0, 0.0).astype(jnp.float32)
        scale = pair[side, cols(q), columns].astype(jnp.float32)
        weighted[side, cols(q), columns] = (scale * (total / (rows * samples) - identity)).astype(jnp.bfloat16)

        @pl.when(p == parts - 1)
        def _():
            theirs_swap(q).start()

    def chain_up(g):
        return remote(second_sent.at[g], below.at[g], sent.at[8], below_recv.at[g], device(row, z + 1))

    def chain_down(g):
        return remote(second_sent.at[g], above.at[g], sent.at[8], above_recv.at[g], device(row, z - 1))

    def spread(g):
        q, i, h = split(g)
        return remote(second_sent.at[g], second_out.at[half(h), cols(q)], sent.at[9], whole.at[4],
                      device(choose(i, targets), z))

    def via(g):
        q, i, h = split(g)
        return remote(second_sent.at[g], passing.at[q, pick(i, [over for over, _ in targets]) - 1], sent.at[9],
                      pass_recv.at[q, pick(i, [over for over, _ in targets]) - 1],
                      device(block_of(0, pick(i, [down for _, down in targets])), z))

    passes = passing.shape[0]

    def pass_on(q, over):
        return remote(passing.at[q, over - 1], second_out.at[half(HALVES - 1), cols(q)], sent.at[11], whole.at[4],
                      device(block_of(over, 0), z))

    middle = jnp.logical_and(a == lax.rem(z, wide), b != lax.div(z, wide))

    from_below = jnp.logical_and(z > 0, z <= row)
    from_above = jnp.logical_and(z < rows - 1, z >= row)

    def second_piece(g):
        q, i, h = split(g)
        target = choose(i, targets)
        contract = (((1,), (1,)), ((), ()))
        second_sum[...] = (
            lax.dot_general(one[0, target, half(h)], weighted[0, cols(q)], contract, preferred_element_type=jnp.float32)
            + lax.dot_general(one[1, target, half(h)], weighted[1, cols(q)], contract,
                              preferred_element_type=jnp.float32))

        @pl.when(from_below)
        def _():
            arrived(below.at[g], below_recv.at[g])
            second_sum[...] += below[g].astype(jnp.float32)

        @pl.when(from_above)
        def _():
            arrived(above.at[g], above_recv.at[g])
            second_sum[...] += above[g].astype(jnp.float32)

        keep = jnp.logical_and(home, i == rows - 1)

        second_sent[g] = second_sum[...].astype(jnp.bfloat16)

        @pl.when(keep)
        def _():
            pltpu.make_async_copy(second_sent.at[g], second_out.at[half(h), cols(q)], whole.at[4]).start()

        @pl.when(z < row)
        def _():
            chain_up(g).start()

        @pl.when(z > row)
        def _():
            chain_down(g).start()

        turned_off = jnp.logical_and(jnp.logical_and(h == HALVES - 1, i < len(far)), q < passes)

        @pl.when(jnp.logical_and(home, turned_off))
        def _():
            via(g).start()

        @pl.when(jnp.logical_and(home, jnp.logical_not(jnp.logical_or(turned_off, i == rows - 1))))
        def _():
            spread(g).start()

    lead = [(0, over, down) for over, _ in across for down in range(deep)]
    lead_deep = [(1, over, down) for _, down in along for over in range(wide)]
    order = []
    for i in range(max(len(lead), len(lead_deep))):
        order += lead[::-1][i:i + 1] + lead_deep[::-1][i:i + 1]
    opening = len(order)
    order += [(0, 0, down) for _, down in along] + [(1, over, 0) for over, _ in across] + [(0, 0, 0), (1, 0, 0)]

    def unit(u):
        h = pick(u, [entry[0] for entry in order])
        over = pick(u, [entry[1] for entry in order])
        down = pick(u, [entry[2] for entry in order])
        return h, over, down, block_of(over, down)

    def first_hop(u):
        h, over, down, target = unit(u)
        flat = jnp.where(h == 0, (over - 1) * deep + lax.div(target, wide), (down - 1) * wide + lax.rem(target, wide))
        return h, over, down, target, flat

    def wide_open(u):
        h, over, down, target, flat = first_hop(u)
        return remote(first_sent.at[target, half(h)], first_wide.at[flat], sent.at[10], wide_recv.at[flat],
                      (b * wide + lax.rem(a + over, wide), col))

    def deep_open(u):
        h, over, down, target, flat = first_hop(u)
        return remote(first_sent.at[target, half(h)], first_deep.at[flat], sent.at[10], deep_recv.at[flat],
                      (lax.rem(b + down, deep) * wide + a, col))

    def deep_close(u):
        h, over, down, target = unit(u)
        return remote(first_sent.at[target, half(h)], deep_sum.at[down - 1], sent.at[10], deep_last.at[down - 1],
                      (target, col))

    def wide_close(u):
        h, over, down, target = unit(u)
        return remote(first_sent.at[target, half(h)], wide_sum.at[over - 1], sent.at[10], wide_last.at[over - 1],
                      (target, col))

    def first_tile(target, h, columns):
        return (jnp.dot(two_own[target, half(h)], weighted[core, :, columns], preferred_element_type=jnp.float32)
                + jnp.dot(two_twin[target, half(h)], theirs[:, columns], preferred_element_type=jnp.float32))

    def first_opening(u):
        h, over, down, target = unit(u)

        def body(i, _):
            columns = at(i * tile, tile)
            first_sent[target, half(h), columns] = first_tile(target, h, columns).astype(jnp.bfloat16)
            return 0

        lax.fori_loop(0, tiles, body, 0)

        @pl.when(h == 0)
        def _():
            wide_open(u).start()

        @pl.when(h == 1)
        def _():
            deep_open(u).start()

    def first_closing(u):
        h, over, down, target = unit(u)

        @pl.when(h == 0)
        def _():
            for over_ in range(1, wide):
                flat = (over_ - 1) * deep + lax.div(target, wide)
                arrived(first_wide.at[flat], wide_recv.at[flat])

        @pl.when(h == 1)
        def _():
            for down_ in range(1, deep):
                flat = (down_ - 1) * wide + lax.rem(target, wide)
                arrived(first_deep.at[flat], deep_recv.at[flat])

        def body(i, _):
            columns = at(i * tile, tile)
            total = first_tile(target, h, columns)

            @pl.when(h == 0)
            def _():
                acc = total
                for over_ in range(1, wide):
                    acc += first_wide[(over_ - 1) * deep + lax.div(target, wide), :, columns].astype(jnp.float32)
                first_sent[target, half(h), columns] = acc.astype(jnp.bfloat16)

            @pl.when(h == 1)
            def _():
                acc = total
                for down_ in range(1, deep):
                    acc += first_deep[(down_ - 1) * wide + lax.rem(target, wide), :, columns].astype(jnp.float32)
                first_sent[target, half(h), columns] = acc.astype(jnp.bfloat16)

            return 0

        lax.fori_loop(0, tiles, body, 0)

        @pl.when(h == 0)
        def _():
            deep_close(u).start()

        @pl.when(h == 1)
        def _():
            wide_close(u).start()

    def first_last():
        for _, down in along:
            arrived(deep_sum.at[down - 1], deep_last.at[down - 1])
        for over, _ in across:
            arrived(wide_sum.at[over - 1], wide_last.at[over - 1])
            for d in range(deep):
                @pl.when(d == b)
                def _(over=over, d=d):
                    flat = (over - 1) * deep + d
                    arrived(first_wide.at[flat], wide_recv.at[flat])
        for _, down in along:
            for o in range(wide):
                @pl.when(o == a)
                def _(down=down, o=o):
                    flat = (down - 1) * wide + o
                    arrived(first_deep.at[flat], deep_recv.at[flat])

        def finish_first(i, _):
            columns = at(i * tile, tile)
            top = first_own[half(0), columns]
            for over, _ in across:
                top += first_wide[(over - 1) * deep + b, :, columns].astype(jnp.float32)
            for _, down in along:
                top += deep_sum[down - 1, :, columns].astype(jnp.float32)
            first_sent[row, half(0), columns] = top.astype(jnp.bfloat16)
            low = first_own[half(1), columns]
            for _, down in along:
                low += first_deep[(down - 1) * wide + a, :, columns].astype(jnp.float32)
            for over, _ in across:
                low += wide_sum[over - 1, :, columns].astype(jnp.float32)
            first_sent[row, half(1), columns] = low.astype(jnp.bfloat16)
            return 0

        lax.fori_loop(0, tiles, finish_first, 0)
        pltpu.make_async_copy(first_sent.at[row], first_out, load_sem.at[3]).start()

    closing = len(order) - 2 - opening
    def run(q, order):
        return [q * chunk + sources.index(pair) * HALVES + h for pair in order for h in range(HALVES)]

    table = run(0, sources)
    ends = [chunk - 1]
    for q in range(1, strips):
        if q <= 2:
            for owned in [1] if q == 1 else range(2, strips):
                table += run(owned, [(0, 0)])
        table += run(q, sources[1:])
        ends.append(len(table) - 1)
    shift = max(end - (q + 1) * chunk + 1 for q, end in enumerate(ends))
    soon = jnp.logical_and(back == 1, jnp.logical_not(last))
    def starts(first_lag, later_lag, length):
        found = []
        for q, end in enumerate(ends):
            begin = end + (later_lag if q else first_lag)
            if q + 1 == strips:
                begin = end + (length > 1)
            found.append(max(begin, found[-1] + length) if found else begin)
        return found

    kinds = [starts(0, 0, 1), starts(4, 0, (parts + 1) // 2), starts(6, 2, (parts + 1) // 2), [ends[0] + 14]]
    kinds[3] += [max(ends[min(2, strips - 1)], kinds[3][0]) + q for q in range(1, strips - 1)]
    kinds[3].append(max(ends[-1], kinds[3][-1] + 1))

    def by_kind(values):
        return jnp.where(last, values[0], jnp.where(soon, values[1], jnp.where(home, values[3], values[2])))

    per = by_kind([parts, 2, 2, parts])
    span = by_kind([1, (parts + 1) // 2, (parts + 1) // 2, 1])
    home_lag = max(kinds[3][0] + 2, chunk + 4 * (rows - 1))
    second_lag = jnp.where(last, chunk - 1, jnp.where(home, home_lag, chunk + 4 * back))
    second_slot = by_kind([kind[0] for kind in kinds]) + jnp.where(jnp.logical_or(last, home), 0, span)
    open_slot = by_kind([kind[-1] for kind in kinds]) + 2
    open_limit = max(kind[-1] for kind in kinds) + 1 + opening
    close_slot = open_limit + by_kind([6, 4, 6, 9])
    relay_slot = pick(jnp.abs(z - row), [8, 4, 2] + [1] * rows)
    feed_slot = chunk + 1 - jnp.minimum(jnp.abs(z - row), 4)
    slots = pieces + 1 + home_lag + shift
    last_slot = slots - 1
    each = (opening + 1) // 2

    def slot(t, _):
        @pl.when(t == relay_slot)
        def _():
            relay_one()

        for q_ in range(2, strips):
            @pl.when(t == feed_slot + (q_ - 2) * (chunk - HALVES))
            def _(q_=q_):
                feeds(q_)

        for q_ in detours[1:]:
            @pl.when(jnp.logical_and(helper, t == ends[q_ - 1]))
            def _(q_=q_):
                hand_over(q_)

        @pl.when(t < pieces)
        def _():
            n = pick(t, table)
            arrived(two_piece(n), two_recv.at[n])

            @pl.when(jnp.logical_and(z >= row, z < rows - 1))
            def _():
                two_up(n).start()

            @pl.when(jnp.logical_and(z <= row, z > 0))
            def _():
                two_down(n).start()

            for q_ in range(strips):
                @pl.when(t == ends[q_])
                def _(q_=q_):
                    two_swap(q_).start()

        @pl.when(t == by_kind([chunk - 2, chunk + 1, chunk + 2, kinds[3][0] - 2]))
        def _():
            take_more()

        @pl.when(t == by_kind([kind[0] for kind in kinds]))
        def _():
            finish_one()

        q, low, high = jnp.int32(0), jnp.int32(0), jnp.int32(0)
        for q_ in range(strips - 1):
            since = t - by_kind([kind[q_] for kind in kinds])
            live = jnp.logical_and(since >= 0, since < span)
            q = jnp.where(live, q_, q)
            low = jnp.where(live, since * per, low)
            high = jnp.where(live, jnp.minimum(since * per + per, parts), high)

        final = t == by_kind([kind[-1] for kind in kinds])
        q = jnp.where(final, strips - 1, q)
        low = jnp.where(final, 0, low)
        high = jnp.where(final, parts, high)

        def piece(i, _):
            correlate(q, i)
            return 0

        lax.fori_loop(low, high, piece, 0)

        @pl.when(t == open_slot)
        def _():
            arrived(two_twin, whole.at[0])
            arrived(theirs, whole.at[2])

        def second_count(t):
            ahead = t - second_lag + 1
            count = jnp.maximum(jnp.minimum(ahead, 2 * chunk), ahead - shift)
            count = jnp.maximum(count, jnp.where(soon, jnp.minimum(ahead + 1, chunk), 0))
            burst = 2 * (t - ends[-1] + 1)
            for end in ends[:-1]:
                burst = jnp.maximum(burst, 0) + jnp.where(t >= end, chunk, 0)
            count = jnp.where(last, burst, count)
            return jnp.where(t < second_slot, 0, jnp.clip(count, 0, pieces))

        def second(g, _):
            second_piece(g)
            return 0

        lax.fori_loop(second_count(t - 1), second_count(t), second, 0)

        turn = t - open_slot
        first = jnp.where(turn > 0, turn + 1, 0)
        final = jnp.where(jnp.logical_and(turn >= 0, turn < opening - 1), turn + 2, first)

        def opener(u, _):
            first_opening(u)
            return 0

        lax.fori_loop(first, final, opener, 0)

        def closer(u, _):
            first_closing(u)
            return 0

        turn = t - close_slot
        first = opening + turn
        final = jnp.where(jnp.logical_and(turn >= 0, turn < closing), first + 1, first)
        lax.fori_loop(first, final, closer, 0)
        turn = t - open_slot - opening

        @pl.when(jnp.logical_and(turn >= 0, turn < HALVES * tiles))
        def _():
            h, columns = lax.div(turn, tiles), at(lax.rem(turn, tiles) * tile, tile)
            first_own[half(h), columns] = first_tile(row, h, columns)

        for q_ in range(passes):
            @pl.when(jnp.logical_and(middle, t == home_lag + q_ * chunk + HALVES + shift + 3))
            def _(q_=q_):
                for over, _ in across:
                    arrived(passing.at[q_, over - 1], pass_recv.at[q_, over - 1])
                    pass_on(q_, over).start()

        @pl.when(t == last_slot)
        def _():
            first_last()

        return 0

    lax.fori_loop(0, slots, slot, 0)

    arrived(second_out, whole.at[4])
    arrived(first_out, load_sem.at[3])

    @pl.when(z != row)
    def _():
        arrived(two_held, sent.at[2])
        arrived(second_sent, sent.at[8])

    @pl.when(home)
    def _():
        arrived(second_sent.at[pl.ds(0, pieces - strips * HALVES)], sent.at[9])

    @pl.when(middle)
    def _():
        arrived(passing, sent.at[11])

    @pl.when(helper)
    def _():
        arrived(handed, sent.at[12])

    @pl.when(jnp.logical_and(z >= row, z < rows - 1))
    def _():
        arrived(two_own, sent.at[0])

    @pl.when(jnp.logical_and(z <= row, z > 0))
    def _():
        arrived(two_own, sent.at[1])

    arrived(two_own, sent.at[3])
    arrived(one.at[core], sent.at[4])
    arrived(weighted.at[other], sent.at[5])
    arrived(pair.at[core], sent.at[6])
    arrived(one.at[core, pl.ds(0, len(across + along))], sent.at[7])
    for block, h, target, i in relays():
        relay(block, h, target, i).wait_send()

    arrived(first_sent.at[pl.ds(0, rows - 1)], sent.at[10])


def settle_kernel(first_ref, second_ref, first_out, second_out, first, second, load, store):
    pairs = ((first_ref, first, first_out), (second_ref, second, second_out))
    part = first_ref.shape[0] // QUARTERS

    def copy(which, i, out):
        source, held, target = pairs[which]
        here = pl.ds(i * part, part)
        if out:
            return pltpu.make_async_copy(held.at[here], target.at[here], store.at[which, i])
        return pltpu.make_async_copy(source.at[here], held.at[here], load.at[which, i])

    order = [(which, i) for i in range(QUARTERS) for which in range(2)]
    for which, i in order:
        copy(which, i, False).start()
    for which, i in order:
        copy(which, i, False).wait()
        copy(which, i, True).start()
    for which, i in order:
        copy(which, i, True).wait()


def settle(first, second):
    any_space = pl.BlockSpec(memory_space=pl.ANY)
    dma = pltpu.SemaphoreType.DMA
    return pl.pallas_call(
        settle_kernel,
        out_shape=[jax.ShapeDtypeStruct(x.shape, x.dtype) for x in (first, second)],
        in_specs=[any_space] * 2,
        out_specs=[any_space] * 2,
        scratch_shapes=[pltpu.VMEM(x.shape, x.dtype) for x in (first, second)] + [dma((2, QUARTERS))] * 2,
        name="settle_grads",
    )(first, second)


def per_device(view_one, view_two, pair_weights):
    rows = lax.axis_size("row")
    samples, width = view_one.shape
    strip = min(width, 256)
    strips = width // strip
    wide, deep = PAIR, rows // PAIR
    part = samples // HALVES
    pieces = strips * rows * HALVES
    passes = max(1, strips - 1)
    own = jax.ShapeDtypeStruct((samples, width), jnp.bfloat16)
    any_space = pl.BlockSpec(memory_space=pl.ANY)
    dma = pltpu.SemaphoreType.DMA

    def held(*shape):
        return pltpu.VMEM(shape, jnp.bfloat16)

    crossing = (wide - 1) * deep
    descent = (deep - 1) * wide
    first, second = pl.pallas_call(
        lambda *refs: step_kernel(rows, strip, *refs),
        out_shape=(own, own),
        in_specs=[any_space] * 3,
        out_specs=(any_space, any_space),
        scratch_shapes=[
            held(samples, width),
            held(rows, samples, width),
            held(rows, samples, width),
            held(strip, rows * samples),
            held(CORES, rows, samples, width),
            held(CORES, width, width),
            held(CORES, width, width),
            held(width, width),
            held(pieces, part, strip),
            held(pieces, part, strip),
            held(pieces, part, strip),
            pltpu.VMEM((part, strip), jnp.float32),
            held(rows, samples, width),
            held(crossing, part, width),
            held(descent, part, width),
            held(wide - 1, part, width),
            held(deep - 1, part, width),
            pltpu.VMEM((samples, width), jnp.float32),
            held(passes, wide - 1, part, strip),
            held((strips + 1) // 2, deep - 1, samples, strip),
            dma((4,)),
            dma((pieces,)),
            dma((rows, HALVES, max(wide, deep) - 1)),
            dma((rows, HALVES)),
            dma((pieces,)),
            dma((pieces,)),
            dma((crossing,)),
            dma((descent,)),
            dma((wide - 1,)),
            dma((deep - 1,)),
            dma((passes, wide - 1)),
            dma(((strips + 1) // 2, deep - 1, HALVES)),
            dma((13,)),
            dma((5,)),
        ],
        compiler_params=pltpu.CompilerParams(collective_id=0, has_side_effects=True, vmem_limit_bytes=62 * 2**20),
        name="twins_step",
    )(view_one, view_two, pair_weights)
    return settle(first, second)


def solution(mesh):
    placed = (P("row", "col"), P("row", "col"), P("row", "col"))
    return jax.shard_map(
        per_device,
        mesh=mesh,
        in_specs=placed,
        out_specs=(P("row", "col"), P("row", "col")),
        check_vma=False,
    )
```
